256 devices in a mesh: strip: 64 (over y, z, core), chan: 4 (over x).
Axes of the slice: x: 4, y: 4, z: 8, core: 2. Of those that a mesh axis runs over, the one named last changes fastest.
Arguments:
- activations: bfloat16 [512, 128, 1280], P('strip', None, 'chan'), may hold values from -17 to 17
- weight: bfloat16 [9, 1280, 1280], P(None, None, 'chan'), may hold values from -0.0546875 to 0.0546875
- gamma: float32 [1280], replicated, may hold values from 0.25 to 1.75
- beta: float32 [1280], replicated, may hold values from -3 to 3
- group_map: int32 [1280], replicated, may hold values from 0 to 31, as said below
- lengths: int32 [64], P('strip'), may hold values from 1 to 8, 384 in all
- stale_edges: bfloat16 [128, 128, 1280], P('strip', None, 'chan'), may hold values from -6 to 6
- stale_mean: float32 [32], replicated, may hold values from -0.5 to 0.5
- stale_square: float32 [32], replicated, may hold values from 1 to 4
- old_mean: float32 [64, 32], P('strip'), may hold values from -0.5 to 0.5
- old_square: float32 [64, 32], P('strip'), may hold values from 0.5 to 6
Outputs:
- upsampled: bfloat16 [1024, 256, 1280], P('strip', None, 'chan')
- new_mean: float32 [32], replicated
- new_square: float32 [32], replicated
The draws below stay inside these ranges and needn't reach their ends.
Inputs may be any that keep to these rules, and one draw needn't show every extreme that they name: `group_map`: every group has exactly 40 channels. The lengths sum to 384, and some strip uses all 8 rows.
All inputs are finite; a program needn't handle non-finite values. No bound on the sum of `lengths` on one device may be relied on, other than what follows from the above.
Results may differ from the reference program's by a relative error of at most 0.0027.
Values may be sent and summed in bfloat16 or wider, within the bound.
A program may use at most 64 MiB of HBM per device.

```python
import math
import jax
import jax.numpy as jnp
import numpy as np
from jax import lax

C = 1280
G = 32
ROWS_DEV = 8
WIDTH = 128
HEIGHT = 512
N_STRIP = 64


def draw_activations(key, part):
    first, second = jax.random.split(key, 2)
    position = jnp.arange(HEIGHT, dtype=jnp.float32) / (HEIGHT - 1)
    noise = jnp.clip(jax.random.normal(first, (HEIGHT, WIDTH, C), jnp.float32), -5.0, 5.0)
    offset = jax.random.uniform(second, (C,), jnp.float32, -1.0, 1.0)
    spread = 1.0 + 2.0 * position
    return (noise * spread[:, None, None] + offset[None, None, :]).astype(jnp.bfloat16)


def draw_group_map(key, part):
    order = jax.random.permutation(key, C)
    return (order // (C // G)).astype(jnp.int32)


def steps_of(rng, shape, cuts, low, top_value):
    level, own = 1.0, jax.random.fold_in(rng, 6)
    for axis_at, blocks in cuts:
        draws = jnp.exp(jax.random.uniform(jax.random.fold_in(own, axis_at), (blocks,), jnp.float32, low / len(cuts), top_value / len(cuts)))
        level = level * jnp.repeat(draws, shape[axis_at] // blocks).reshape([-1 if axis == axis_at else 1 for axis in range(len(shape))])
    return level


def length_profile(count, total, bound, slope):
    loads = [(1 << 20) // math.isqrt(standing ** slope) + 1 for standing in range(2, count + 1)]
    surplus, counts = total - bound - (count - 1), [1] * (count - 1)
    while surplus > 0:
        free = [i for i in range(count - 1) if counts[i] < bound]
        pool, remaining = sum([loads[i] for i in free]), surplus
        for i in free:
            extra = min(bound - counts[i], max(1, remaining * loads[i] // pool), surplus)
            counts[i] = counts[i] + extra
            surplus = surplus - extra
    return np.array([bound] + counts)


def uneven_parts(own_key, amount, total, most, lean):
    if amount == 2:
        one = jax.random.randint(own_key, (), max(1, total - most), min(most, total - 1) + 1)
        return jnp.stack([one, total - one])
    sizes = jnp.asarray(length_profile(amount, total, most, lean), jnp.int32)
    pairs = (amount - 1) // 2
    donor, taker = sizes[1:1 + 2 * pairs:2], sizes[2:2 + 2 * pairs:2]
    margin = jnp.minimum(donor - 1, most - taker)
    shifted = jax.random.randint(jax.random.fold_in(own_key, 1), (pairs,), 0, 1 << 20) % (margin + 1)
    sizes = sizes.at[1:1 + 2 * pairs:2].set(donor - shifted).at[2:2 + 2 * pairs:2].set(taker + shifted)
    return sizes[jax.random.permutation(jax.random.fold_in(own_key, 2), amount)]


def scatter_about(stream_key, extent, scale, bound, pieces=(), kind=jnp.bfloat16):
    drawn = scale * jax.random.normal(stream_key, extent, jnp.float32)
    if pieces:
        drawn = drawn * steps_of(stream_key, extent, pieces, -0.22, 0.18)
    return jnp.clip(drawn, -bound, bound).astype(kind)


def setup_inputs(seed: int = 0) -> dict:
    seeds = jax.random.split(jax.random.key(seed), 12)
    return {
        "activations": draw_activations(jax.random.fold_in(seeds[11], 71), 0),
        "weight": scatter_about(seeds[1], (9, C, C), (9 * C) ** -0.5, 0.0546875, ((2, 4),)),
        "gamma": jnp.clip(1.0 + 0.15 * jax.random.normal(seeds[2], (C,), jnp.float32), 0.25, 1.75),
        "beta": scatter_about(seeds[3], (C,), 0.7, 3.0, (), jnp.float32),
        "group_map": draw_group_map(jax.random.fold_in(seeds[11], 71), 0),
        "lengths": uneven_parts(seeds[5], N_STRIP, N_STRIP * (3 * ROWS_DEV // 4), ROWS_DEV, 2).astype(jnp.int32),
        "stale_edges": scatter_about(seeds[6], (2 * N_STRIP, WIDTH, C), 1.0, 6.0, ((0, 64), (2, 4))),
        "stale_mean": jnp.clip(jax.random.uniform(seeds[7], (G,), jnp.float32, -0.5, 0.5), -0.5, 0.5),
        "stale_square": jnp.clip(jax.random.uniform(seeds[8], (G,), jnp.float32, 1.0, 4.0), 1.0, 4.0),
        "old_mean": jnp.clip(jax.random.uniform(seeds[9], (N_STRIP, G), jnp.float32, -0.5, 0.5) * steps_of(seeds[9], (N_STRIP, G), ((0, 64),), -0.4, 0.0), -0.5, 0.5),
        "old_square": jnp.clip(0.5 + 5.5 * jax.random.uniform(seeds[10], (N_STRIP, G), jnp.float32) ** steps_of(seeds[10], (N_STRIP, G), ((0, 64),), -0.2, 0.2), 0.5, 6.0),
    }


EPS = 1e-05

def reference(activations, weight, gamma, beta, group_map, lengths, stale_edges, stale_mean, stale_square, old_mean, old_square):
    per_group = C // G
    grid = activations.reshape(N_STRIP, ROWS_DEV, WIDTH, C)
    member = (group_map[:, None] == jnp.arange(G, dtype=jnp.int32)[None, :]).astype(jnp.float32)
    used = (jnp.arange(ROWS_DEV, dtype=jnp.int32)[None, :] < lengths[:, None]).astype(jnp.float32)
    values = grid.astype(jnp.float32) * used[:, :, None, None]
    chan_sum = lax.optimization_barrier(jnp.sum(values, axis=(1, 2)))
    chan_sq = lax.optimization_barrier(jnp.sum(values * values, axis=(1, 2)))
    sum_one = lax.optimization_barrier(jnp.sum(chan_sum[:, :, None] * member[None], axis=1))
    sum_two = lax.optimization_barrier(jnp.sum(chan_sq[:, :, None] * member[None], axis=1))
    count = (lengths.astype(jnp.float32) * (WIDTH * per_group))[:, None]
    fresh_mean = sum_one / count
    fresh_square = sum_two / count
    mean_g = stale_mean[None] + fresh_mean - old_mean
    square_g = stale_square[None] + fresh_square - old_square
    var_g = jnp.maximum(square_g - mean_g * mean_g, 0.5 * (fresh_square - fresh_mean * fresh_mean))
    rstd_g = lax.rsqrt(var_g + EPS)
    scale_c = lax.optimization_barrier(jnp.sum(member[None] * rstd_g[:, None, :], axis=2)) * gamma[None]
    shift_c = beta[None] - lax.optimization_barrier(jnp.sum(member[None] * mean_g[:, None, :], axis=2)) * scale_c
    edges = stale_edges.reshape(N_STRIP, 2, WIDTH, C)
    zero_row = jnp.zeros((1, WIDTH, C), jnp.bfloat16)
    upper = jnp.concatenate([zero_row, edges[:-1, 1]], axis=0)
    lower = jnp.concatenate([edges[1:, 0], zero_row], axis=0)

    def one_strip(items):
        strip_x, scale, shift, mask, above, below, length = items
        maskb = mask[:, None, None]
        act = (jax.nn.silu(strip_x.astype(jnp.float32) * scale + shift) * maskb).astype(jnp.bfloat16)
        padded = jnp.concatenate([above[None], act, jnp.zeros((1, WIDTH, C), jnp.bfloat16)], axis=0)
        place = (jnp.arange(ROWS_DEV + 2, dtype=jnp.int32) == length + 1)[:, None, None]
        padded = jnp.where(place, below[None], padded)
        padded = jnp.pad(padded, ((0, 0), (1, 1), (0, 0)))
        total = jnp.zeros((ROWS_DEV * WIDTH, C), jnp.float32)
        for tap in range(9):
            dy, dx = (tap // 3, tap % 3)
            patch = padded[dy:dy + ROWS_DEV, dx:dx + WIDTH].reshape(ROWS_DEV * WIDTH, C)
            total = total + jnp.dot(patch, weight[tap], preferred_element_type=jnp.float32)
        block = (strip_x.astype(jnp.float32) + total.reshape(ROWS_DEV, WIDTH, C)) * maskb
        return block.astype(jnp.bfloat16)
    blocks = lax.map(one_strip, (grid, scale_c, shift_c, used, upper, lower, lengths))
    blocks = blocks.reshape(HEIGHT, WIDTH, C)
    upsampled = jnp.repeat(jnp.repeat(blocks, 2, axis=0), 2, axis=1)
    total_count = float(N_STRIP * (3 * ROWS_DEV // 4) * WIDTH * per_group)
    new_mean = lax.optimization_barrier(jnp.sum(sum_one, axis=0)) / total_count
    new_square = lax.optimization_barrier(jnp.sum(sum_two, axis=0)) / total_count
    return (upsampled, new_mean, new_square)
```

```python
import functools

import jax
import jax.numpy as jnp
from jax import lax
from jax.experimental import pallas as pl
from jax.experimental.pallas import tpu as pltpu
from jax.sharding import PartitionSpec as P

EPS = 1e-05
F32 = jnp.float32
BF16 = jnp.bfloat16
MAIN = 256
REM = 64
LANES = 128
KEY = 1024


def torus(strips):
    return {64: (4, 8), 4: (1, 2)}[strips]


def silu(v):
    return v / (1.0 + jnp.exp(-v))


def exact_dot(a, b, contract):
    return lax.dot_general(
        a, b, (contract, ((), ())), precision=lax.Precision.HIGHEST, preferred_element_type=F32
    )


def main_kernel(
    rows, width, strips, chans, per_group,
    act_hbm, edge_hbm, weight_hbm, params,
    block_out, moments_out,
    araw, ebuf, raw, feats, wts, acc, affine, st_own, st_chan, st_core, st_z, st_y,
    load_sem, wt_sem, own_send, own_recv, fwd_send, fwd_recv, edge_send, edge_recv,
    stat_send, chan_recv, core_recv, z_recv, y_recv,
):
    ny, nz = torus(strips)
    pairs = rows // 2
    edge = pairs
    x = lax.axis_index("chan")
    s = lax.axis_index("strip")
    core = s % 2
    z = (s // 2) % nz
    y = s // (2 * nz)
    right, left, far = (x + 1) % chans, (x + 3) % chans, (x + 2) % chans
    above, below = (s + strips - 1) % strips, (s + 1) % strips

    def to_z(k):
        return (y * nz + (z + k) % nz) * 2 + core

    def to_y(k):
        return (((y + k) % ny) * nz + z) * 2 + core

    partner = s + 1 - 2 * core

    loads = []
    for c in range(pairs):
        copy = pltpu.make_async_copy(
            act_hbm.at[pl.ds(2 * c, 2)], araw.at[pl.ds(2 * c, 2)], load_sem.at[c]
        )
        copy.start()
        loads.append(copy)

    barrier = pltpu.get_barrier_semaphore()
    greeted = 0
    for target in (right, left, far):
        pl.semaphore_signal(barrier, inc=1, device_id={"chan": target})
        greeted += 1
    others = [partner, above, below]
    others += [to_z(k) for k in range(1, nz)] + [to_y(k) for k in range(1, ny)]
    for target in others:
        pl.semaphore_signal(barrier, inc=1, device_id={"strip": target})
        greeted += 1

    slabs = (x, left, right, far)
    for j in range(chans):
        start = slabs[j] * (MAIN + REM)
        for dy in range(3):
            for dx in range(3):
                pltpu.make_async_copy(
                    weight_hbm.at[3 * dy + dx, pl.ds(pl.multiple_of(start, REM), MAIN)],
                    wts.at[dy, j, pl.ds(dx * MAIN, MAIN)],
                    wt_sem.at[j],
                ).start()
                pltpu.make_async_copy(
                    weight_hbm.at[3 * dy + dx, pl.ds(pl.multiple_of(start + MAIN, REM), REM)],
                    wts.at[dy, j, pl.ds(3 * MAIN + dx * REM, REM)],
                    wt_sem.at[j],
                ).start()
    tail = KEY - 3 * (MAIN + REM)
    for j in range(chans):
        for dy in range(3):
            wts[dy, j, pl.ds(KEY - tail, tail)] = jnp.zeros((tail, MAIN + REM), BF16)

    lane = lax.broadcasted_iota(jnp.int32, (1, LANES), 1)
    first_half = lane < REM
    length = params[16:17, 0:LANES]

    ones = [jnp.zeros((8, LANES), F32) for _ in range(3)]
    twos = [jnp.zeros((8, LANES), F32) for _ in range(3)]

    def fold(v):
        return jnp.sum(v.reshape(width // 8, 8, LANES), axis=0)

    for c in range(pairs):
        loads[c].wait()
        raw[0, c, :, 0:MAIN] = araw[2 * c, :, 0:MAIN]
        raw[0, c, :, MAIN:2 * MAIN] = araw[2 * c + 1, :, 0:MAIN]
        rem = jnp.concatenate(
            [araw[2 * c, :, MAIN:MAIN + REM], araw[2 * c + 1, :, MAIN:MAIN + REM]], axis=1
        )
        raw[0, c, :, 2 * MAIN:2 * MAIN + LANES] = rem
        for t in range(5):
            v = raw[0, c, :, t * LANES:(t + 1) * LANES].astype(F32)
            if t < 4:
                row = (2 * c + t // 2) + jnp.zeros((1, LANES), F32)
            else:
                row = 2 * c + jnp.where(first_half, 0.0, 1.0)
            mask = jnp.where(row < length, 1.0, 0.0)
            at = t % 2 if t < 4 else 2
            ones[at] = ones[at] + fold(v) * mask
            twos[at] = twos[at] + fold(v * v) * mask
    sums = jnp.concatenate(
        [jnp.concatenate(ones, axis=1), jnp.concatenate(twos, axis=1)], axis=0
    )

    def member(slab):
        return (
            params[pl.ds(8 + slab, 1), :]
            == lax.broadcasted_iota(jnp.int32, (LANES, MAIN + LANES), 0).astype(F32)
        ).astype(F32)

    by_group = exact_dot(sums, member(x), ((1,), (1,)))
    own = jnp.concatenate(
        [
            jnp.sum(by_group[0:8], axis=0, keepdims=True),
            jnp.sum(by_group[8:16], axis=0, keepdims=True),
            jnp.zeros((6, LANES), F32),
        ],
        axis=0,
    )
    st_own[0] = own
    st_chan[x] = own

    pl.semaphore_wait(barrier, greeted)

    sends = []

    def send(src, dst, send_sem, recv_sem, target):
        copy = pltpu.make_async_remote_copy(
            src_ref=src, dst_ref=dst, send_sem=send_sem, recv_sem=recv_sem,
            device_id=target, device_id_type=pl.DeviceIdType.MESH,
        )
        copy.start()
        sends.append(copy)

    def wait_for(dst, sem):
        pltpu.make_async_copy(dst, dst, sem).wait()

    for k in range(1, chans):
        send(
            st_own.at[0], st_chan.at[x], stat_send.at[k - 1], chan_recv.at[k - 1],
            {"chan": (x + k) % chans},
        )

    def send_own(c):
        send(raw.at[0, c], raw.at[1, c], own_send.at[0, c], own_recv.at[0, c], {"chan": right})
        send(raw.at[0, c], raw.at[2, c], own_send.at[1, c], own_recv.at[1, c], {"chan": left})

    send(edge_hbm.at[0], ebuf.at[1], edge_send.at[0], edge_recv.at[1], {"strip": above})
    send(edge_hbm.at[1], ebuf.at[0], edge_send.at[1], edge_recv.at[0], {"strip": below})
    send_own(0)
    send_own(1)

    wait_for(ebuf.at[0], edge_recv.at[0])
    wait_for(ebuf.at[1], edge_recv.at[1])
    keep_upper = jnp.where(s > 0, 1.0, 0.0).astype(BF16)
    keep_lower = jnp.where(s < strips - 1, 1.0, 0.0).astype(BF16)
    raw[0, edge, :, 0:MAIN] = ebuf[0, :, 0:MAIN] * keep_upper
    raw[0, edge, :, MAIN:2 * MAIN] = ebuf[1, :, 0:MAIN] * keep_lower
    raw[0, edge, :, 2 * MAIN:2 * MAIN + LANES] = jnp.concatenate(
        [ebuf[0, :, MAIN:MAIN + REM] * keep_upper, ebuf[1, :, MAIN:MAIN + REM] * keep_lower], axis=1
    )

    for k in range(1, chans):
        wait_for(st_chan.at[(x + chans - k) % chans], chan_recv.at[k - 1])
    strip_sum = st_chan[0]
    for k in range(1, chans):
        strip_sum = strip_sum + st_chan[k]
    st_own[1] = strip_sum
    st_core[core] = strip_sum
    count = length * float(width * per_group)
    fresh_mean = strip_sum[0:1] / count
    fresh_square = strip_sum[1:2] / count
    mean = params[12:13, 0:LANES] + fresh_mean - params[14:15, 0:LANES]
    square = params[13:14, 0:LANES] + fresh_square - params[15:16, 0:LANES]
    var = jnp.maximum(square - mean * mean, 0.5 * (fresh_square - fresh_mean * fresh_mean))
    rstd = lax.rsqrt(var + EPS)
    both = jnp.concatenate([rstd, mean, jnp.zeros((6, LANES), F32)], axis=0)
    for j in range(chans):
        spread = exact_dot(both, member(slabs[j]), ((1,), (0,)))
        scale = spread[0:1] * params[pl.ds(slabs[j], 1), :]
        shift = params[pl.ds(4 + slabs[j], 1), :] - spread[1:2] * scale
        affine[j, 0:1] = scale
        affine[j, 1:2] = shift

    send_own(edge)
    for c in range(2, pairs):
        send_own(c)
    send(
        st_own.at[1], st_core.at[core], stat_send.at[3], core_recv.at[0], {"strip": partner}
    )

    at_row = lax.broadcasted_iota(jnp.int32, (width, 1), 0)

    def shifted(a):
        before = jnp.where(at_row == 0, 0.0, pltpu.roll(a, 1, 0))
        after = jnp.where(at_row == width - 1, 0.0, pltpu.roll(a, width - 1, 0))
        return before, a, after

    def store_main(j, p, t, a):
        for dx, v in enumerate(shifted(a)):
            feats[j, p, :, dx * MAIN + t * LANES:dx * MAIN + (t + 1) * LANES] = v.astype(BF16)

    def store_rem(j, p_one, p_two, a):
        before, same, after = shifted(a)
        turned = [pltpu.roll(v, REM, 1) for v in (before, same, after)]
        base = 3 * MAIN
        feats[j, p_one, :, base:base + LANES] = jnp.where(first_half, before, turned[1]).astype(BF16)
        feats[j, p_one, :, base + LANES:base + 2 * LANES] = jnp.where(first_half, after, 0.0).astype(BF16)
        feats[j, p_two, :, base:base + LANES] = jnp.where(first_half, turned[0], same).astype(BF16)
        feats[j, p_two, :, base + LANES:base + 2 * LANES] = jnp.where(first_half, turned[2], 0.0).astype(BF16)

    def tile(j, c, t):
        return raw[j, c, :, t * LANES:(t + 1) * LANES].astype(F32)

    def prepare(j, c):
        def picked(row, t, low):
            at = t % 2 if t < 4 else 2
            lanes = slice(at * LANES, (at + 1) * LANES)
            v = tile(j, c, t) * affine[j, 0:1, lanes] + affine[j, 1:2, lanes]
            return jnp.where(row < length, silu(v), jnp.where(row == length, low, 0.0))

        first = (2 * c + jnp.zeros((1, LANES), jnp.int32)).astype(F32)
        for h in range(2):
            for t in range(2):
                a = picked(first + float(h), 2 * h + t, tile(j, edge, 2 + t))
                store_main(j, 2 * c + h + 1, t, a)
        borders = tile(j, edge, 4)
        low = jnp.where(first_half, pltpu.roll(borders, REM, 1), borders)
        store_rem(j, 2 * c + 1, 2 * c + 2, picked(first + jnp.where(first_half, 0.0, 1.0), 4, low))

    def prepare_edge(j):
        full = float(rows) == length
        for t in range(2):
            store_main(j, 0, t, tile(j, edge, t))
            store_main(j, rows + 1, t, jnp.where(full, tile(j, edge, 2 + t), 0.0))
        borders = tile(j, edge, 4)
        store_rem(j, 0, rows + 1, jnp.where(first_half | full, borders, 0.0))

    def product(j, pair, dy):
        patch = feats[j, pl.ds(2 * pair + dy, 2)].reshape(2 * width, KEY)
        return jnp.dot(patch, wts[dy, j], preferred_element_type=F32)

    def conv(j, pair, first=False):
        total = product(j, pair, 0) + product(j, pair, 1) + product(j, pair, 2)
        acc[pair] = total if first else acc[pair] + total

    def wait_weights(j):
        landed = wts.at[:, j, pl.ds(0, 3 * (MAIN + REM))]
        pltpu.make_async_copy(landed, landed, wt_sem.at[j]).wait()

    prepare_edge(0)

    @pl.loop(0, pairs)
    def _(c):
        prepare(0, c)

    wait_for(st_core.at[1 - core], core_recv.at[0])
    chip_sum = st_core[0] + st_core[1]
    st_own[2] = chip_sum
    st_z[z] = chip_sum
    wait_weights(0)

    @pl.loop(0, pairs // 2)
    def _(pair):
        conv(0, pair, first=True)

    for k in range(1, nz):
        send(st_own.at[2], st_z.at[z], stat_send.at[3 + k], z_recv.at[k - 1], {"strip": to_z(k)})

    @pl.loop(pairs // 2, pairs)
    def _(pair):
        conv(0, pair, first=True)

    def got(c):
        wait_for(raw.at[1, c], own_recv.at[0, c])
        wait_for(raw.at[2, c], own_recv.at[1, c])

    def forward(direction, c, at, half=None):
        src, dst = raw.at[1 + direction, c], raw.at[3, c]
        if half is not None:
            part = pl.ds(half * (width // 2), width // 2)
            src, dst = src.at[part], dst.at[part]
        send(
            src, dst, fwd_send.at[direction, at], fwd_recv.at[direction, at],
            {"chan": (right, left)[direction]},
        )

    def got_far(direction, c, at, half=None):
        dst = raw.at[3, c]
        if half is not None:
            dst = dst.at[pl.ds(half * (width // 2), width // 2)]
        wait_for(dst, fwd_recv.at[direction, at])

    got(0)
    got(1)
    got(edge)
    forward(0, edge, 0)
    forward(1, 1, 0)
    forward(0, 0, 1)
    wait_weights(1)
    wait_weights(2)

    @pl.loop(1, 3)
    def _(j):
        prepare_edge(j)
        prepare(j, 0)
        prepare(j, 1)
        conv(j, 0)

    for k in range(1, nz):
        wait_for(st_z.at[(z + nz - k) % nz], z_recv.at[k - 1])
    line_sum = st_z[0]
    for k in range(1, nz):
        line_sum = line_sum + st_z[k]
    st_own[3] = line_sum
    st_y[y] = line_sum
    got(2)
    forward(1, 2, 1)
    for k in range(1, ny):
        send(
            st_own.at[3], st_y.at[y], stat_send.at[2 + nz + k], y_recv.at[k - 1],
            {"strip": to_y(k)},
        )

    @pl.loop(1, 3)
    def _(j):
        prepare(j, 2)
        conv(j, 1)

    got(3)
    forward(0, 3, 2, half=0)
    forward(1, 3, 2, half=1)

    @pl.loop(1, 3)
    def _(j):
        prepare(j, 3)
        conv(j, 2)
        conv(j, 3)

    for k in range(1, ny):
        wait_for(st_y.at[(y + ny - k) % ny], y_recv.at[k - 1])
    image_sum = st_y[0]
    for k in range(1, ny):
        image_sum = image_sum + st_y[k]
    moments_out[...] = image_sum / float(strips * (3 * rows // 4) * width * per_group)

    wait_weights(3)
    got_far(0, edge, 0)
    got_far(1, 1, 0)
    prepare_edge(3)
    prepare(3, 1)
    got_far(0, 0, 1)
    got_far(1, 2, 1)

    @pl.loop(0, 2)
    def _(i):
        prepare(3, 2 * i)

    @pl.loop(0, 2)
    def _(pair):
        conv(3, pair)

    got_far(0, 3, 2, half=0)
    got_far(1, 3, 2, half=1)
    prepare(3, 3)

    @pl.loop(2, pairs)
    def _(pair):
        conv(3, pair)

    @pl.loop(0, rows)
    def _(r):
        at = (r % 2) * width
        total = acc[r // 2, pl.ds(pl.multiple_of(at, width), width)]
        value = araw[r].astype(F32) + total
        row = (r + jnp.zeros((1, 1), jnp.int32)).astype(F32)
        block_out[r] = jnp.where(row < length[:, 0:1], value, 0.0).astype(BF16)

    for copy in sends:
        copy.wait_send()


def spread_kernel(rows, width, local, block, moments, up_hbm, mean_out, square_out, buf, sem):
    twice = (
        lax.broadcasted_iota(jnp.int32, (2 * width, width), 0) // 2
        == lax.broadcasted_iota(jnp.int32, (2 * width, width), 1)
    ).astype(F32).astype(BF16)
    copies = []
    for r in range(rows):
        wide = jnp.dot(twice, block[r], preferred_element_type=F32).astype(BF16)
        buf[2 * r] = wide
        buf[2 * r + 1] = wide
        copy = pltpu.make_async_copy(
            buf.at[pl.ds(2 * r, 2)], up_hbm.at[pl.ds(2 * r, 2)], sem.at[r]
        )
        copy.start()
        copies.append(copy)
    groups = mean_out.shape[1]
    mean_out[...] = moments[0:1, 0:groups]
    square_out[...] = moments[1:2, 0:groups]
    for copy in copies:
        copy.wait()


def per_device(
    activations, weight, gamma, beta, group_map, lengths, stale_edges,
    stale_mean, stale_square, old_mean, old_square,
):
    rows, width, local = activations.shape
    channels = weight.shape[1]
    groups = stale_mean.shape[0]
    strips, chans = lax.axis_size("strip"), lax.axis_size("chan")
    ny, nz = torus(strips)
    pairs = rows // 2

    wide = MAIN + LANES

    def slabs(v):
        v = v.astype(F32).reshape(chans, local)
        return jnp.concatenate([v, v[:, MAIN:]], axis=1)

    def moment(v):
        return jnp.pad(v.reshape(1, groups), ((0, 0), (0, wide - groups)))

    params = jnp.concatenate(
        [
            slabs(gamma), slabs(beta), slabs(group_map),
            moment(stale_mean), moment(stale_square), moment(old_mean), moment(old_square),
            jnp.broadcast_to(lengths.astype(F32)[:, None], (8, wide)),
        ],
        axis=0,
    )

    dma = pltpu.SemaphoreType.DMA
    any_space = pl.BlockSpec(memory_space=pl.ANY)
    vmem = pl.BlockSpec(memory_space=pltpu.VMEM)
    flops = 2 * rows * width * 9 * channels * local
    block, moments = pl.pallas_call(
        functools.partial(main_kernel, rows, width, strips, chans, channels // groups),
        name="gather_conv",
        out_shape=(
            jax.ShapeDtypeStruct((rows, width, local), BF16),
            jax.ShapeDtypeStruct((8, LANES), F32),
        ),
        in_specs=[any_space, any_space, any_space, vmem],
        out_specs=(vmem, vmem),
        scratch_shapes=[
            pltpu.VMEM((rows, width, local), BF16),
            pltpu.VMEM((2, width, local), BF16),
            pltpu.VMEM((chans, pairs + 1, width, 2 * MAIN + LANES), BF16),
            pltpu.VMEM((chans, rows + 2, width, KEY), BF16),
            pltpu.VMEM((3, chans, KEY, local), BF16),
            pltpu.VMEM((pairs, 2 * width, local), F32),
            pltpu.VMEM((chans, 8, wide), F32),
            pltpu.VMEM((4, 8, LANES), F32),
            pltpu.VMEM((chans, 8, LANES), F32),
            pltpu.VMEM((2, 8, LANES), F32),
            pltpu.VMEM((nz, 8, LANES), F32),
            pltpu.VMEM((ny, 8, LANES), F32),
            dma((pairs,)),
            dma((chans,)),
            dma((2, pairs + 1)),
            dma((2, pairs + 1)),
            dma((2, 3)),
            dma((2, 3)),
            dma((2,)),
            dma((2,)),
            dma((3 + nz + ny,)),
            dma((chans - 1,)),
            dma((1,)),
            dma((max(nz - 1, 1),)),
            dma((max(ny - 1, 1),)),
        ],
        compiler_params=pltpu.CompilerParams(
            collective_id=0, has_side_effects=True, vmem_limit_bytes=56 * 1024 * 1024
        ),
        cost_estimate=pl.CostEstimate(
            flops=flops, bytes_accessed=weight.size * 2, transcendentals=rows * width * channels
        ),
    )(activations, stale_edges, weight, params)

    upsampled, new_mean, new_square = pl.pallas_call(
        functools.partial(spread_kernel, rows, width, local),
        name="spread",
        out_shape=(
            jax.ShapeDtypeStruct((2 * rows, 2 * width, local), BF16),
            jax.ShapeDtypeStruct((1, groups), F32),
            jax.ShapeDtypeStruct((1, groups), F32),
        ),
        in_specs=[vmem, vmem],
        out_specs=(any_space, vmem, vmem),
        scratch_shapes=[pltpu.VMEM((2 * rows, 2 * width, local), BF16), dma((rows,))],
        compiler_params=pltpu.CompilerParams(vmem_limit_bytes=32 * 1024 * 1024),
    )(block, moments)
    return upsampled, new_mean.reshape(groups), new_square.reshape(groups)


def solution(mesh):
    in_specs = (
        P("strip", None, "chan"),
        P(None, None, "chan"),
        P(),
        P(),
        P(),
        P("strip"),
        P("strip", None, "chan"),
        P(),
        P(),
        P("strip", None),
        P("strip", None),
    )
    out_specs = (P("strip", None, "chan"), P(), P())
    return jax.shard_map(
        per_device, mesh=mesh, in_specs=in_specs, out_specs=out_specs, check_vma=False
    )
```

```python
import functools

import jax
import jax.numpy as jnp
from jax import lax
from jax.experimental import pallas as pl
from jax.experimental.pallas import tpu as pltpu
from jax.sharding import PartitionSpec as P

EPS = 1e-05
F32 = jnp.float32
BF16 = jnp.bfloat16
MAIN = 256
REM = 64
SLAB = MAIN + REM
LANES = 128


def torus(strips):
    return {64: (4, 8), 4: (1, 2)}[strips]


def main_kernel(
    rows, width, strips, chans, per_group,
    act_hbm, edge_hbm, weight_hbm, gamma, beta, groups_of, lengths,
    stale_mean, stale_square, old_mean, old_square,
    block_hbm, moments_out,
    raw, feats, feats_rem, wts, wts_rem, acc, block, columns, group_col, affine,
    st_own, st_chan, st_core, st_z, st_y,
    load_sem, wt_sem, own_send, own_recv, fwd_send, fwd_recv, edge_send, edge_recv,
    stat_send, chan_recv, core_recv, z_recv, y_recv, out_sem,
):
    ny, nz = torus(strips)
    pairs = rows // 2
    tiles = chans * SLAB // LANES
    x = lax.axis_index("chan")
    s = lax.axis_index("strip")
    core = s % 2
    z = (s // 2) % nz
    y = s // (2 * nz)
    right, left, far = (x + 1) % chans, (x + 3) % chans, (x + 2) % chans
    above, below = (s + strips - 1) % strips, (s + 1) % strips
    partner = s + 1 - 2 * core
    slabs = (x, left, right, far)

    def slab_of(j):
        return (x + (j % 2) * ((7 - j) // 2) + (1 - j % 2) * (j // 2)) % chans

    def to_z(k):
        return (y * nz + (z + k) % nz) * 2 + core

    def to_y(k):
        return (((y + k) % ny) * nz + z) * 2 + core

    loads = []
    for c in range(pairs):
        copy = pltpu.make_async_copy(
            act_hbm.at[pl.ds(2 * c, 2)], raw.at[0, pl.ds(2 * c, 2)], load_sem.at[c]
        )
        copy.start()
        loads.append(copy)

    barrier = pltpu.get_barrier_semaphore()
    greeted = 0
    for target in (right, left, far):
        pl.semaphore_signal(barrier, inc=1, device_id={"chan": target})
        greeted += 1
    others = [partner, above, below]
    others += [to_z(k) for k in range(1, nz)] + [to_y(k) for k in range(1, ny)]
    for target in others:
        pl.semaphore_signal(barrier, inc=1, device_id={"strip": target})
        greeted += 1

    def main_start(slab):
        return pl.multiple_of(SLAB * slab + REM * (slab % 2), LANES)

    for j in range(chans):
        for dy in range(3):
            for dx in range(3):
                pltpu.make_async_copy(
                    weight_hbm.at[3 * dy + dx, :, pl.ds(main_start(slabs[j]), MAIN)],
                    wts.at[dy, j, :, pl.ds(dx * MAIN, MAIN)],
                    wt_sem.at[j],
                ).start()
    for g in range(2):
        first = pl.multiple_of(MAIN + 2 * SLAB * ((x // 2 + g) % 2), LANES)
        for dy in range(3):
            for dx in range(3):
                pltpu.make_async_copy(
                    weight_hbm.at[3 * dy + dx, :, pl.ds(first, LANES)],
                    wts_rem.at[dy, g, :, pl.ds(dx * LANES, LANES)],
                    wt_sem.at[chans + g],
                ).start()

    lane = lax.broadcasted_iota(jnp.int32, (1, LANES), 1)
    length = jnp.full((1, LANES), lengths[0], jnp.int32)

    columns[...] = jnp.transpose(
        jnp.concatenate(
            [
                gamma[...], beta[...], groups_of[...].astype(F32),
                jnp.zeros((LANES - 3 * tiles, LANES), F32),
            ],
            axis=0,
        )
    )
    for t in range(tiles):
        group_col[t * LANES:(t + 1) * LANES] = jnp.broadcast_to(
            columns[:, 2 * tiles + t:2 * tiles + t + 1], (LANES, LANES)
        ).astype(jnp.int32)

    for copy in loads:
        copy.wait()
    group_one = jnp.zeros((1, LANES), F32)
    group_two = jnp.zeros((1, LANES), F32)
    for i in range(SLAB // REM):
        one = jnp.zeros((REM, LANES), F32)
        two = jnp.zeros((REM, LANES), F32)
        for q in range(rows):
            v = jnp.where(q < length, raw[0, q, i * REM:(i + 1) * REM, :].astype(F32), 0.0)
            one = one + v
            two = two + v * v
        own_at = pl.ds(pl.multiple_of(SLAB * x + REM * i, REM), REM)
        member = group_col[own_at] == lane
        chan_one = jnp.sum(one, axis=1, keepdims=True)
        chan_two = jnp.sum(two, axis=1, keepdims=True)
        group_one = group_one + jnp.sum(jnp.where(member, chan_one, 0.0), axis=0, keepdims=True)
        group_two = group_two + jnp.sum(jnp.where(member, chan_two, 0.0), axis=0, keepdims=True)
    own = jnp.concatenate([group_one, group_two, jnp.zeros((6, LANES), F32)], axis=0)
    st_own[0] = own
    st_chan[x] = own

    pl.semaphore_wait(barrier, greeted)

    sends = []

    def send(src, dst, send_sem, recv_sem, target):
        copy = pltpu.make_async_remote_copy(
            src_ref=src, dst_ref=dst, send_sem=send_sem, recv_sem=recv_sem,
            device_id=target, device_id_type=pl.DeviceIdType.MESH,
        )
        copy.start()
        sends.append(copy)

    def wait_for(dst, sem):
        pltpu.make_async_copy(dst, dst, sem).wait()

    edge = pairs

    def pair_of(j, c):
        return raw.at[j, pl.ds(2 * c, 2)]

    def send_own(c):
        for d, target in enumerate((right, left)):
            send(
                pair_of(0, c), pair_of(1 + d, c), own_send.at[d, c], own_recv.at[d, c],
                {"chan": target},
            )

    for k in range(1, chans):
        send(
            st_own.at[0], st_chan.at[x], stat_send.at[k - 1], chan_recv.at[k - 1],
            {"chan": (x + k) % chans},
        )
    send(edge_hbm.at[0], raw.at[0, rows + 1], edge_send.at[0], edge_recv.at[1], {"strip": above})
    send(edge_hbm.at[1], raw.at[0, rows], edge_send.at[1], edge_recv.at[0], {"strip": below})
    send_own(0)
    send_own(1)
    wait_for(raw.at[0, rows], edge_recv.at[0])
    wait_for(raw.at[0, rows + 1], edge_recv.at[1])
    send_own(edge)
    send_own(2)
    send_own(3)

    for k in range(1, chans):
        wait_for(st_chan.at[(x + chans - k) % chans], chan_recv.at[k - 1])
    strip_sum = st_chan[0]
    for k in range(1, chans):
        strip_sum = strip_sum + st_chan[k]
    st_own[1] = strip_sum
    st_core[core] = strip_sum
    groups = stale_mean.shape[1]

    def padded(ref):
        return jnp.concatenate([ref[...], jnp.zeros((1, LANES - groups), F32)], axis=1)

    count = length.astype(F32) * float(width * per_group)
    fresh_mean = strip_sum[0:1] / count
    fresh_square = strip_sum[1:2] / count
    mean = padded(stale_mean) + fresh_mean - padded(old_mean)
    square = padded(stale_square) + fresh_square - padded(old_square)
    var = jnp.maximum(square - mean * mean, 0.5 * (fresh_square - fresh_mean * fresh_mean))
    rstd = lax.rsqrt(var + EPS)
    for t in range(tiles):
        at = slice(t * LANES, (t + 1) * LANES)
        member = group_col[at] == lane
        rstd_c = jnp.sum(jnp.where(member, rstd, 0.0), axis=1, keepdims=True)
        mean_c = jnp.sum(jnp.where(member, mean, 0.0), axis=1, keepdims=True)
        scale = rstd_c * columns[:, t:t + 1]
        shift = columns[:, tiles + t:tiles + t + 1] - mean_c * scale
        affine[0, at] = jnp.broadcast_to(0.5 * scale, (LANES, LANES))
        affine[1, at] = jnp.broadcast_to(0.5 * shift, (LANES, LANES))
    send(
        st_own.at[1], st_core.at[core], stat_send.at[3], core_recv.at[0], {"strip": partner}
    )

    is_first = lane == 0
    is_last = lane == width - 1
    top = jnp.full((1, LANES), s, jnp.int32) > 0
    bottom = jnp.full((1, LANES), s, jnp.int32) < strips - 1

    def store(j, i, p, a):
        before = jnp.where(is_first, 0.0, pltpu.roll(a, 1, 1)).astype(BF16)
        after = jnp.where(is_last, 0.0, pltpu.roll(a, width - 1, 1)).astype(BF16)
        cells = pl.ds(pl.multiple_of(p * width, LANES), width)
        if i < MAIN // REM:
            for dx, v in enumerate((before, a.astype(BF16), after)):
                feats[j, dx * MAIN + i * REM:dx * MAIN + (i + 1) * REM, cells] = v
        else:
            slab = slab_of(j)
            g = (slab // 2 + x // 2) % 2
            for dx, v in enumerate((before, a.astype(BF16), after)):
                at = pl.ds(pl.multiple_of(dx * LANES + REM * (slab % 2), REM), REM)
                feats_rem[g, at, cells] = v

    def piece(j, i):
        odd = slab_of(j) % 2
        if i < MAIN // REM:
            return REM * i + REM * odd
        return MAIN * (1 - odd)

    def at_piece(start):
        return pl.ds(pl.multiple_of(start, REM), REM)

    def prepare(j, q):
        row = jnp.zeros((1, LANES), jnp.int32) + q
        for i in range(SLAB // REM):
            start = piece(j, i)
            total = at_piece(SLAB * slab_of(j) + start)
            h = raw[j, q, at_piece(start), :].astype(F32) * affine[0, total] + affine[1, total]
            a = h + h * jnp.tanh(h)
            low = raw[j, rows + 1, at_piece(start), :].astype(F32)
            low = jnp.where((row == length) & bottom, low, 0.0)
            store(j, i, q + 1, jnp.where(row < length, a, low))

    def prepare_edge(j):
        for i in range(SLAB // REM):
            start = piece(j, i)
            high = raw[j, rows, at_piece(start), :].astype(F32)
            store(j, i, 0, jnp.where(top, high, 0.0))
            low = raw[j, rows + 1, at_piece(start), :].astype(F32)
            store(j, i, rows + 1, jnp.where((length == rows) & bottom, low, 0.0))

    def prepare_pair(j, c):
        prepare(j, 2 * c)
        prepare(j, 2 * c + 1)

    def cells_of(pair, dy):
        return pl.ds(pl.multiple_of((2 * pair + dy) * width, LANES), 2 * width)

    def term(j, pair, dy):
        return jnp.dot(wts[dy, j], feats[j, :, cells_of(pair, dy)], preferred_element_type=F32)

    def term_rem(g, pair, dy):
        return jnp.dot(
            wts_rem[dy, g], feats_rem[g, :, cells_of(pair, dy)], preferred_element_type=F32
        )

    def add_to(pair, total, first=False):
        at = pl.ds(pl.multiple_of(pair * 2 * width, LANES), 2 * width)
        acc[:, at] = total if first else acc[:, at] + total

    def conv(j, pair, first=False):
        add_to(pair, term(j, pair, 0) + term(j, pair, 1) + term(j, pair, 2), first)

    def conv_rem(g, pair):
        add_to(pair, term_rem(g, pair, 0) + term_rem(g, pair, 1) + term_rem(g, pair, 2))

    def wait_weights(j):
        pltpu.make_async_copy(wts.at[:, j], wts.at[:, j], wt_sem.at[j]).wait()

    def wait_weights_rem(g):
        pltpu.make_async_copy(wts_rem.at[:, g], wts_rem.at[:, g], wt_sem.at[chans + g]).wait()

    prepare_edge(0)

    @pl.loop(0, rows)
    def _(q):
        prepare(0, q)

    wait_for(st_core.at[1 - core], core_recv.at[0])
    chip_sum = st_core[0] + st_core[1]
    st_own[2] = chip_sum
    st_z[z] = chip_sum
    wait_weights(0)

    @pl.loop(0, pairs // 2)
    def _(pair):
        conv(0, pair, first=True)

    for k in range(1, nz):
        send(st_own.at[2], st_z.at[z], stat_send.at[3 + k], z_recv.at[k - 1], {"strip": to_z(k)})

    @pl.loop(pairs // 2, pairs)
    def _(pair):
        conv(0, pair, first=True)

    def got(c):
        for d in range(2):
            wait_for(pair_of(1 + d, c), own_recv.at[d, c])

    def forward(d, at, first, number):
        part = pl.ds(first, number)
        send(
            raw.at[1 + d, part], raw.at[3, part], fwd_send.at[d, at], fwd_recv.at[d, at],
            {"chan": (right, left)[d]},
        )

    def got_far(d, at, first, number):
        wait_for(raw.at[3, pl.ds(first, number)], fwd_recv.at[d, at])

    plan = (
        ((rows, 2), (0, 2), (6, 1)),
        ((2, 2), (4, 2), (7, 1)),
    )

    got(0)
    got(1)
    forward(1, 0, *plan[1][0])
    got(edge)
    forward(0, 0, *plan[0][0])
    forward(0, 1, *plan[0][1])
    wait_weights(1)
    wait_weights(2)

    @pl.loop(1, 3)
    def _(j):
        prepare_edge(j)
        prepare_pair(j, 0)
        prepare_pair(j, 1)
        conv(j, 0)

    for k in range(1, nz):
        wait_for(st_z.at[(z + nz - k) % nz], z_recv.at[k - 1])
    line_sum = st_z[0]
    for k in range(1, nz):
        line_sum = line_sum + st_z[k]
    st_own[3] = line_sum
    st_y[y] = line_sum
    got(2)
    forward(1, 1, *plan[1][1])
    for k in range(1, ny):
        send(
            st_own.at[3], st_y.at[y], stat_send.at[2 + nz + k], y_recv.at[k - 1],
            {"strip": to_y(k)},
        )

    @pl.loop(1, 3)
    def _(j):
        prepare_pair(j, 2)
        conv(j, 1)

    got(3)
    forward(0, 2, *plan[0][2])
    forward(1, 2, *plan[1][2])

    @pl.loop(1, 3)
    def _(j):
        prepare_pair(j, 3)
        conv(j, 2)
        conv(j, 3)

    wait_weights_rem(0)

    @pl.loop(0, pairs)
    def _(pair):
        conv_rem(0, pair)

    for k in range(1, ny):
        wait_for(st_y.at[(y + ny - k) % ny], y_recv.at[k - 1])
    image_sum = st_y[0]
    for k in range(1, ny):
        image_sum = image_sum + st_y[k]
    moments_out[...] = image_sum / float(strips * (3 * rows // 4) * width * per_group)

    wait_weights(3)
    wait_weights_rem(1)
    got_far(0, 0, *plan[0][0])
    got_far(1, 0, *plan[1][0])
    prepare_edge(3)
    prepare_pair(3, 1)
    got_far(0, 1, *plan[0][1])
    got_far(1, 1, *plan[1][1])

    outs = []

    def finish(pair):
        for h in range(2):
            r = 2 * pair + h
            value = raw[0, r].astype(F32) + acc[:, r * width:(r + 1) * width]
            block[r] = jnp.where(r < length, value, 0.0).astype(BF16)

    def put(pair):
        at = pl.ds(2 * pair, 2)
        copy = pltpu.make_async_copy(block.at[at], block_hbm.at[at], out_sem.at[pair])
        copy.start()
        outs.append(copy)

    @pl.loop(0, 2)
    def _(i):
        prepare_pair(3, 2 * i)

    @pl.loop(0, 2)
    def _(pair):
        conv(3, pair)
        conv_rem(1, pair)

    finish(0)
    finish(1)
    add_to(2, term(3, 2, 0) + term(3, 2, 1) + term_rem(1, 2, 0) + term_rem(1, 2, 1))
    put(0)
    put(1)
    got_far(0, 2, *plan[0][2])
    got_far(1, 2, *plan[1][2])
    prepare_pair(3, 3)
    add_to(2, term(3, 2, 2) + term_rem(1, 2, 2))
    finish(2)
    put(2)
    conv(3, 3)
    conv_rem(1, 3)
    finish(3)
    put(3)

    for copy in sends:
        copy.wait_send()
    for copy in outs:
        copy.wait()


def spread_kernel(
    rows, width, local, block_hbm, moments, up_hbm, mean_out, square_out, block, buf, in_sem, out_sem
):
    takes = []
    for r in range(0, rows, 2):
        at = pl.ds(r, 2)
        copy = pltpu.make_async_copy(block_hbm.at[at], block.at[at], in_sem.at[r // 2])
        copy.start()
        takes.append(copy)
    twice = (
        lax.broadcasted_iota(jnp.int32, (width, 2 * width), 1) // 2
        == lax.broadcasted_iota(jnp.int32, (width, 2 * width), 0)
    ).astype(F32).astype(BF16)
    groups = mean_out.shape[1]
    mean_out[...] = moments[0:1, 0:groups]
    square_out[...] = moments[1:2, 0:groups]
    puts = []
    for r in range(rows):
        if r % 2 == 0:
            takes[r // 2].wait()
        buf[r] = jnp.dot(block[r], twice, preferred_element_type=F32).astype(BF16)
        for a in range(2):
            copy = pltpu.make_async_copy(buf.at[r], up_hbm.at[2 * r + a], out_sem.at[2 * r + a])
            copy.start()
            puts.append(copy)
    for copy in puts:
        copy.wait()


def per_device(
    activations, weight, gamma, beta, group_map, lengths, stale_edges,
    stale_mean, stale_square, old_mean, old_square,
):
    rows, width, local = activations.shape
    channels = weight.shape[1]
    groups = stale_mean.shape[0]
    strips, chans = lax.axis_size("strip"), lax.axis_size("chan")
    ny, nz = torus(strips)
    pairs = rows // 2

    def turned(v):
        return jnp.swapaxes(v, 1, 2)

    dma = pltpu.SemaphoreType.DMA
    any_space = pl.BlockSpec(memory_space=pl.ANY)
    vmem = pl.BlockSpec(memory_space=pltpu.VMEM)
    smem = pl.BlockSpec(memory_space=pltpu.SMEM)
    flops = 2 * rows * width * 9 * channels * local
    block, moments = pl.pallas_call(
        functools.partial(main_kernel, rows, width, strips, chans, channels // groups),
        name="gather_conv",
        out_shape=(
            jax.ShapeDtypeStruct((rows, local, width), BF16),
            jax.ShapeDtypeStruct((8, LANES), F32),
        ),
        in_specs=[any_space] * 3 + [vmem] * 3 + [smem] + [vmem] * 4,
        out_specs=(any_space, vmem),
        scratch_shapes=[
            pltpu.VMEM((chans, rows + 2, local, width), BF16),
            pltpu.VMEM((chans, 3 * MAIN, (rows + 2) * width), BF16),
            pltpu.VMEM((2, 3 * LANES, (rows + 2) * width), BF16),
            pltpu.VMEM((3, chans, local, 3 * MAIN), BF16),
            pltpu.VMEM((3, 2, local, 3 * LANES), BF16),
            pltpu.VMEM((local, rows * width), F32),
            pltpu.VMEM((rows, local, width), BF16),
            pltpu.VMEM((LANES, LANES), F32),
            pltpu.VMEM((channels, LANES), jnp.int32),
            pltpu.VMEM((2, channels, LANES), F32),
            pltpu.VMEM((4, 8, LANES), F32),
            pltpu.VMEM((chans, 8, LANES), F32),
            pltpu.VMEM((2, 8, LANES), F32),
            pltpu.VMEM((nz, 8, LANES), F32),
            pltpu.VMEM((ny, 8, LANES), F32),
            dma((pairs,)),
            dma((chans + 2,)),
            dma((2, pairs + 1)),
            dma((2, pairs + 1)),
            dma((2, 3)),
            dma((2, 3)),
            dma((2,)),
            dma((2,)),
            dma((3 + nz + ny,)),
            dma((chans - 1,)),
            dma((1,)),
            dma((max(nz - 1, 1),)),
            dma((max(ny - 1, 1),)),
            dma((pairs,)),
        ],
        compiler_params=pltpu.CompilerParams(
            collective_id=0, has_side_effects=True, vmem_limit_bytes=60 * 1024 * 1024
        ),
        cost_estimate=pl.CostEstimate(
            flops=flops, bytes_accessed=weight.size * 2, transcendentals=rows * width * channels
        ),
    )(
        turned(activations), turned(stale_edges), turned(weight),
        gamma.reshape(-1, LANES), beta.reshape(-1, LANES), group_map.reshape(-1, LANES), lengths,
        stale_mean.reshape(1, groups), stale_square.reshape(1, groups), old_mean, old_square,
    )

    upsampled, new_mean, new_square = pl.pallas_call(
        functools.partial(spread_kernel, rows, width, local),
        name="spread",
        out_shape=(
            jax.ShapeDtypeStruct((2 * rows, local, 2 * width), BF16),
            jax.ShapeDtypeStruct((1, groups), F32),
            jax.ShapeDtypeStruct((1, groups), F32),
        ),
        in_specs=[any_space, vmem],
        out_specs=(any_space, vmem, vmem),
        scratch_shapes=[
            pltpu.VMEM((rows, local, width), BF16),
            pltpu.VMEM((rows, local, 2 * width), BF16),
            dma((pairs,)),
            dma((2 * rows,)),
        ],
        compiler_params=pltpu.CompilerParams(vmem_limit_bytes=60 * 1024 * 1024),
    )(block, moments)
    return turned(upsampled), new_mean.reshape(groups), new_square.reshape(groups)


def solution(mesh):
    in_specs = (
        P("strip", None, "chan"),
        P(None, None, "chan"),
        P(),
        P(),
        P(),
        P("strip"),
        P("strip", None, "chan"),
        P(),
        P(),
        P("strip", None),
        P("strip", None),
    )
    out_specs = (P("strip", None, "chan"), P(), P())
    return jax.shard_map(
        per_device, mesh=mesh, in_specs=in_specs, out_specs=out_specs, check_vma=False
    )
```

```python
import functools

import jax
import jax.numpy as jnp
from jax import lax
from jax.experimental import pallas as pl
from jax.experimental.pallas import tpu as pltpu
from jax.sharding import PartitionSpec as P

EPS = 1e-05
F32 = jnp.float32
BF16 = jnp.bfloat16
MAIN = 256
REM = 64
SLAB = MAIN + REM
LANES = 128


def torus(strips):
    return {64: (4, 8), 4: (1, 2)}[strips]


def main_kernel(
    rows, width, strips, chans, per_group,
    act_hbm, edge_hbm, weight_hbm, *rest
):
    (
        gamma_hbm, beta_hbm, groups_hbm, lengths,
        stale_mean_hbm, stale_square_hbm, old_mean_hbm, old_square_hbm,
        block_hbm, moments_hbm,
        gamma, beta, groups_of, stale_mean, stale_square, old_mean, old_square, moments,
        small_sem, hop, raw, feats, feats_rem, wts, wts_rem, acc, block, columns, group_col, affine,
    st_own, st_chan, st_core, st_z, st_y,
    load_sem, wt_sem, own_send, own_recv, fwd_send, fwd_recv, edge_send, edge_recv,
    stat_send, chan_recv, core_recv, z_recv, y_recv, out_sem,
    ) = rest
    ny, nz = torus(strips)
    pairs = rows // 2
    tiles = chans * SLAB // LANES
    x = lax.axis_index("chan")
    s = lax.axis_index("strip")
    core = s % 2
    z = (s // 2) % nz
    y = s // (2 * nz)
    right, left, far = (x + 1) % chans, (x + 3) % chans, (x + 2) % chans
    partner = s + 1 - 2 * core
    z_peer = (y * nz + (z + 2 * core + nz - 1) % nz) * 2 + 1 - core
    turns = z == core * (nz - 1)
    peer_turns = (z + 2 * core + nz - 1) % nz == (1 - core) * (nz - 1)
    slabs = (x, left, right, far)

    def slab_of(j):
        return (x + (j % 2) * ((7 - j) // 2) + (1 - j % 2) * (j // 2)) % chans

    def to_z(k):
        return (y * nz + (z + k) % nz) * 2 + core

    def to_y(k):
        return (((y + k) % ny) * nz + z) * 2 + core

    loads = []
    for c in range(pairs):
        copy = pltpu.make_async_copy(
            act_hbm.at[pl.ds(2 * c, 2)], raw.at[0, pl.ds(2 * c, 2)], load_sem.at[c]
        )
        copy.start()
        loads.append(copy)

    small = []
    for i, (src, dst) in enumerate(
        (
            (gamma_hbm, gamma), (beta_hbm, beta), (groups_hbm, groups_of),
            (stale_mean_hbm, stale_mean), (stale_square_hbm, stale_square),
            (old_mean_hbm, old_mean), (old_square_hbm, old_square),
        )
    ):
        copy = pltpu.make_async_copy(src, dst, small_sem.at[i])
        copy.start()
        small.append(copy)

    barrier = pltpu.get_barrier_semaphore()
    greeted = 0
    for target in (right, left, far):
        pl.semaphore_signal(barrier, inc=1, device_id={"chan": target})
        greeted += 1
    others = [partner, z_peer] + [to_y(k) for k in range(1, ny)]
    for target in others:
        pl.semaphore_signal(barrier, inc=1, device_id={"strip": target})
        greeted += 1

    def main_start(slab):
        return pl.multiple_of(SLAB * slab + REM * (slab % 2), LANES)

    for j in range(chans):
        for dy in range(3):
            for dx in range(3):
                pltpu.make_async_copy(
                    weight_hbm.at[3 * dy + dx, :, pl.ds(main_start(slabs[j]), MAIN)],
                    wts.at[dy, j, :, pl.ds(dx * MAIN, MAIN)],
                    wt_sem.at[j],
                ).start()
    for g in range(2):
        first = pl.multiple_of(MAIN + 2 * SLAB * ((x // 2 + g) % 2), LANES)
        for dy in range(3):
            for dx in range(3):
                pltpu.make_async_copy(
                    weight_hbm.at[3 * dy + dx, :, pl.ds(first, LANES)],
                    wts_rem.at[dy, g, :, pl.ds(dx * LANES, LANES)],
                    wt_sem.at[chans + g],
                ).start()

    lane = lax.broadcasted_iota(jnp.int32, (1, LANES), 1)
    length = jnp.full((1, LANES), lengths[0], jnp.int32)

    for copy in small:
        copy.wait()
    columns[...] = jnp.transpose(
        jnp.concatenate(
            [
                gamma[...], beta[...], groups_of[...].astype(F32),
                jnp.zeros((LANES - 3 * tiles, LANES), F32),
            ],
            axis=0,
        )
    )
    for t in range(tiles):
        group_col[t * LANES:(t + 1) * LANES] = jnp.broadcast_to(
            columns[:, 2 * tiles + t:2 * tiles + t + 1], (LANES, LANES)
        ).astype(jnp.int32)

    pl.semaphore_wait(barrier, greeted)

    sends = []

    def send(src, dst, send_sem, recv_sem, target):
        copy = pltpu.make_async_remote_copy(
            src_ref=src, dst_ref=dst, send_sem=send_sem, recv_sem=recv_sem,
            device_id=target, device_id_type=pl.DeviceIdType.MESH,
        )
        copy.start()
        sends.append(copy)

    def wait_for(dst, sem):
        pltpu.make_async_copy(dst, dst, sem).wait()

    edge = pairs

    def pair_of(j, c):
        return raw.at[j, pl.ds(2 * c, 2)]

    def send_own(c):
        for d, target in enumerate((right, left)):
            send(
                pair_of(0, c), pair_of(1 + d, c), own_send.at[d, c], own_recv.at[d, c],
                {"chan": target},
            )

    for copy in loads:
        copy.wait()
    send_own(0)
    send(
        edge_hbm.at[1 - core], raw.at[0, rows + core], edge_send.at[0], edge_recv.at[0],
        {"strip": partner},
    )

    @pl.when(peer_turns)
    def _():
        pltpu.make_async_remote_copy(
            src_ref=edge_hbm.at[core], dst_ref=hop, send_sem=edge_send.at[1],
            recv_sem=edge_recv.at[1], device_id={"strip": z_peer},
            device_id_type=pl.DeviceIdType.MESH,
        ).start()

    @pl.when(jnp.logical_not(peer_turns))
    def _():
        pltpu.make_async_remote_copy(
            src_ref=edge_hbm.at[core], dst_ref=raw.at[0, rows + 1 - core],
            send_sem=edge_send.at[1], recv_sem=edge_recv.at[1], device_id={"strip": z_peer},
            device_id_type=pl.DeviceIdType.MESH,
        ).start()

    group_one = jnp.zeros((1, LANES), F32)
    group_two = jnp.zeros((1, LANES), F32)
    for i in range(SLAB // REM):
        one = jnp.zeros((REM, LANES), F32)
        two = jnp.zeros((REM, LANES), F32)
        for q in range(rows):
            v = jnp.where(q < length, raw[0, q, i * REM:(i + 1) * REM, :].astype(F32), 0.0)
            one = one + v
            two = two + v * v
        own_at = pl.ds(pl.multiple_of(SLAB * x + REM * i, REM), REM)
        member = group_col[own_at] == lane
        chan_one = jnp.sum(one, axis=1, keepdims=True)
        chan_two = jnp.sum(two, axis=1, keepdims=True)
        group_one = group_one + jnp.sum(jnp.where(member, chan_one, 0.0), axis=0, keepdims=True)
        group_two = group_two + jnp.sum(jnp.where(member, chan_two, 0.0), axis=0, keepdims=True)
    own = jnp.concatenate([group_one, group_two, jnp.zeros((6, LANES), F32)], axis=0)
    st_own[0] = own
    st_chan[x] = own
    for k in range(1, chans):
        send(
            st_own.at[0], st_chan.at[x], stat_send.at[k - 1], chan_recv.at[k - 1],
            {"chan": (x + k) % chans},
        )
    send_own(1)
    wait_for(raw.at[0, rows + 1 - core], edge_recv.at[0])

    @pl.when(turns)
    def _():
        wait_for(hop, edge_recv.at[1])
        pltpu.make_async_remote_copy(
            src_ref=hop, dst_ref=raw.at[0, rows + core], send_sem=edge_send.at[2],
            recv_sem=edge_recv.at[2],
            device_id={"strip": ((y + 1 + core * (ny - 2)) % ny * nz + z) * 2 + core},
            device_id_type=pl.DeviceIdType.MESH,
        ).start()
        wait_for(raw.at[0, rows + core], edge_recv.at[2])

    @pl.when(jnp.logical_not(turns))
    def _():
        wait_for(raw.at[0, rows + core], edge_recv.at[1])

    send_own(edge)
    send_own(2)
    send_own(3)

    for k in range(1, chans):
        wait_for(st_chan.at[(x + chans - k) % chans], chan_recv.at[k - 1])
    strip_sum = st_chan[0]
    for k in range(1, chans):
        strip_sum = strip_sum + st_chan[k]
    st_own[1] = strip_sum
    st_core[core] = strip_sum
    groups = stale_mean.shape[1]

    def padded(ref):
        return jnp.concatenate([ref[...], jnp.zeros((1, LANES - groups), F32)], axis=1)

    count = length.astype(F32) * float(width * per_group)
    fresh_mean = strip_sum[0:1] / count
    fresh_square = strip_sum[1:2] / count
    mean = padded(stale_mean) + fresh_mean - padded(old_mean)
    square = padded(stale_square) + fresh_square - padded(old_square)
    var = jnp.maximum(square - mean * mean, 0.5 * (fresh_square - fresh_mean * fresh_mean))
    rstd = lax.rsqrt(var + EPS)
    for t in range(tiles):
        at = slice(t * LANES, (t + 1) * LANES)
        member = group_col[at] == lane
        rstd_c = jnp.sum(jnp.where(member, rstd, 0.0), axis=1, keepdims=True)
        mean_c = jnp.sum(jnp.where(member, mean, 0.0), axis=1, keepdims=True)
        scale = rstd_c * columns[:, t:t + 1]
        shift = columns[:, tiles + t:tiles + t + 1] - mean_c * scale
        affine[0, at] = jnp.broadcast_to(0.5 * scale, (LANES, LANES))
        affine[1, at] = jnp.broadcast_to(0.5 * shift, (LANES, LANES))
    send(
        st_own.at[1], st_core.at[core], stat_send.at[3], core_recv.at[0], {"strip": partner}
    )

    def flag(condition):
        return jnp.where(condition, 1.0, 0.0).astype(BF16)

    not_first = flag(lane != 0)
    not_last = flag(lane != width - 1)
    top = flag(jnp.full((1, LANES), s, jnp.int32) > 0)
    bottom = jnp.full((1, LANES), s, jnp.int32) < strips - 1

    def store(j, i, p, a):
        before = pltpu.roll(a, 1, 1) * not_first
        after = pltpu.roll(a, width - 1, 1) * not_last
        cells = pl.ds(pl.multiple_of(p * width, LANES), width)
        if i < MAIN // REM:
            for dx, v in enumerate((before, a, after)):
                feats[j, dx * MAIN + i * REM:dx * MAIN + (i + 1) * REM, cells] = v
        else:
            slab = slab_of(j)
            g = (slab // 2 + x // 2) % 2
            for dx, v in enumerate((before, a, after)):
                at = pl.ds(pl.multiple_of(dx * LANES + REM * (slab % 2), REM), REM)
                feats_rem[g, at, cells] = v

    def piece(j, i):
        odd = slab_of(j) % 2
        if i < MAIN // REM:
            return REM * i + REM * odd
        return MAIN * (1 - odd)

    def at_piece(start):
        return pl.ds(pl.multiple_of(start, REM), REM)

    def prepare(j, q):
        row = jnp.zeros((1, LANES), jnp.int32) + q
        in_use = flag(row < length)
        border = flag((row == length) & bottom)
        for i in range(SLAB // REM):
            start = piece(j, i)
            total = at_piece(SLAB * slab_of(j) + start)
            h = raw[j, q, at_piece(start), :].astype(F32) * affine[0, total] + affine[1, total]
            a = (h + h * jnp.tanh(h)).astype(BF16)
            store(j, i, q + 1, a * in_use + raw[j, rows + 1, at_piece(start), :] * border)

    def prepare_edge(j):
        border = flag((length == rows) & bottom)
        for i in range(SLAB // REM):
            start = piece(j, i)
            store(j, i, 0, raw[j, rows, at_piece(start), :] * top)
            store(j, i, rows + 1, raw[j, rows + 1, at_piece(start), :] * border)

    def prepare_pair(j, c):
        prepare(j, 2 * c)
        prepare(j, 2 * c + 1)

    def cells_of(pair, dy):
        return pl.ds(pl.multiple_of((2 * pair + dy) * width, LANES), 2 * width)

    def term(j, pair, dy):
        return jnp.dot(wts[dy, j], feats[j, :, cells_of(pair, dy)], preferred_element_type=F32)

    def term_rem(g, pair, dy):
        return jnp.dot(
            wts_rem[dy, g], feats_rem[g, :, cells_of(pair, dy)], preferred_element_type=F32
        )

    def add_to(pair, total, first=False):
        at = pl.ds(pl.multiple_of(pair * 2 * width, LANES), 2 * width)
        acc[:, at] = total if first else acc[:, at] + total

    def products(pair, steps, slabs_in, groups_in):
        total = None
        for dy in steps:
            for j in slabs_in:
                one = term(j, pair, dy)
                total = one if total is None else total + one
            for g in groups_in:
                total = total + term_rem(g, pair, dy)
        return total

    def wait_weights(j):
        pltpu.make_async_copy(wts.at[:, j], wts.at[:, j], wt_sem.at[j]).wait()

    def wait_weights_rem(g):
        pltpu.make_async_copy(wts_rem.at[:, g], wts_rem.at[:, g], wt_sem.at[chans + g]).wait()

    prepare_edge(0)

    @pl.loop(0, rows)
    def _(q):
        prepare(0, q)

    wait_for(st_core.at[1 - core], core_recv.at[0])
    chip_sum = st_core[0] + st_core[1]
    st_own[2] = chip_sum
    st_z[z] = chip_sum
    wait_weights(0)

    for pair in range(pairs // 2):
        add_to(pair, products(pair, (0, 1, 2), (0,), ()), first=True)

    reach = ((1, nz - 1), (2, nz - 2), tuple(range(3, nz - 2)))
    if nz < 4:
        reach = ((1,), (), ())

    def send_z(step):
        for k in reach[step]:
            send(
                st_own.at[2], st_z.at[z], stat_send.at[3 + k], z_recv.at[k - 1],
                {"strip": to_z(k)},
            )

    def got_z(step):
        for k in reach[step]:
            wait_for(st_z.at[(z + nz - k) % nz], z_recv.at[k - 1])

    send_z(0)

    for pair in range(pairs // 2, pairs):
        add_to(pair, products(pair, (0, 1, 2), (0,), ()), first=True)

    got_z(0)
    send_z(1)

    def got(c):
        for d in range(2):
            wait_for(pair_of(1 + d, c), own_recv.at[d, c])

    plan = [
        [(rows + 1 - d, 0, SLAB)]
        + [(2 * i + d, 0, SLAB) for i in range(pairs - 1)]
        + [(rows - 2, d * (SLAB // 2), SLAB // 2), (rows - 1, d * (SLAB // 2), SLAB // 2)]
        for d in range(2)
    ]

    def forward(d, k):
        q, start, number = plan[d][k]
        part = pl.ds(start, number)
        send(
            raw.at[1 + d, q, part], raw.at[3, q, part], fwd_send.at[d, k], fwd_recv.at[d, k],
            {"chan": (right, left)[d]},
        )

    def got_far(k):
        for d in range(2):
            q, start, number = plan[d][k]
            wait_for(raw.at[3, q, pl.ds(start, number)], fwd_recv.at[d, k])

    got(0)
    got(1)
    got(edge)
    for k in range(3):
        for d in range(2):
            forward(d, k)
    wait_weights(1)
    wait_weights(2)
    wait_weights_rem(0)

    @pl.loop(1, 3)
    def _(j):
        prepare_edge(j)
        prepare_pair(j, 0)
        prepare_pair(j, 1)

    def add_sides(pair, *steps):
        add_to(pair, products(pair, steps, (1, 2), (0,)))

    add_sides(0, 0, 1, 2)
    add_sides(1, 0, 1)
    got_z(1)
    send_z(2)
    got(2)
    for d in range(2):
        forward(d, 3)

    @pl.loop(1, 3)
    def _(j):
        prepare_pair(j, 2)

    add_sides(1, 2)
    add_sides(2, 0, 1)
    got_z(2)
    line_sum = st_z[0]
    for k in range(1, nz):
        line_sum = line_sum + st_z[k]
    st_own[3] = line_sum
    st_y[y] = line_sum
    got(3)
    for k in range(4, 6):
        for d in range(2):
            forward(d, k)
    for k in range(1, ny):
        send(
            st_own.at[3], st_y.at[y], stat_send.at[2 + nz + k], y_recv.at[k - 1],
            {"strip": to_y(k)},
        )

    @pl.loop(1, 3)
    def _(j):
        prepare_pair(j, 3)

    add_sides(2, 2)
    add_sides(3, 0, 1, 2)

    for k in range(1, ny):
        wait_for(st_y.at[(y + ny - k) % ny], y_recv.at[k - 1])
    image_sum = st_y[0]
    for k in range(1, ny):
        image_sum = image_sum + st_y[k]
    moments[...] = image_sum / float(strips * (3 * rows // 4) * width * per_group)

    wait_weights(3)
    wait_weights_rem(1)
    outs = []

    def finish(pair):
        for h in range(2):
            r = 2 * pair + h
            value = raw[0, r].astype(F32) + acc[:, r * width:(r + 1) * width]
            block[r] = jnp.where(r < length, value, 0.0).astype(BF16)

    def put(pair):
        at = pl.ds(2 * pair, 2)
        copy = pltpu.make_async_copy(block.at[at], block_hbm.at[at], out_sem.at[pair])
        copy.start()
        outs.append(copy)

    def both(pair, *steps):
        add_to(pair, products(pair, steps, (3,), (1,)))

    got_far(0)
    prepare_edge(3)
    got_far(1)
    prepare_pair(3, 0)
    both(0, 0, 1)
    got_far(2)
    prepare_pair(3, 1)
    both(0, 2)
    finish(0)
    both(1, 0, 1)
    put(0)
    got_far(3)
    prepare_pair(3, 2)
    both(1, 2)
    finish(1)
    both(2, 0, 1)
    put(1)
    got_far(4)
    prepare(3, rows - 2)
    both(2, 2)
    finish(2)
    both(3, 0)
    put(2)
    got_far(5)
    prepare(3, rows - 1)
    both(3, 1, 2)
    finish(3)
    put(3)

    copy = pltpu.make_async_copy(moments, moments_hbm, small_sem.at[7])
    copy.start()
    outs.append(copy)
    for copy in sends:
        copy.wait_send()
    wait_for(edge_hbm.at[0], edge_send.at[1])

    @pl.when(turns)
    def _():
        wait_for(hop, edge_send.at[2])

    for copy in outs:
        copy.wait()


def spread_kernel(
    rows, width, local, block_hbm, moments_hbm, up_hbm, mean_hbm, square_hbm,
    block, moments, mean_out, square_out, buf, in_sem, out_sem,
):
    takes = []
    for r in range(0, rows, 2):
        at = pl.ds(r, 2)
        copy = pltpu.make_async_copy(block_hbm.at[at], block.at[at], in_sem.at[r // 2])
        copy.start()
        takes.append(copy)
    take = pltpu.make_async_copy(moments_hbm, moments, in_sem.at[rows // 2])
    take.start()
    twice = (
        lax.broadcasted_iota(jnp.int32, (width, 2 * width), 1) // 2
        == lax.broadcasted_iota(jnp.int32, (width, 2 * width), 0)
    ).astype(F32).astype(BF16)
    puts = []
    for r in range(rows):
        if r % 2 == 0:
            takes[r // 2].wait()
        buf[r] = jnp.dot(block[r], twice, preferred_element_type=F32).astype(BF16)
        for a in range(2):
            copy = pltpu.make_async_copy(buf.at[r], up_hbm.at[2 * r + a], out_sem.at[2 * r + a])
            copy.start()
            puts.append(copy)
    groups = mean_out.shape[1]
    take.wait()
    mean_out[...] = moments[0:1, 0:groups]
    square_out[...] = moments[1:2, 0:groups]
    for i, (src, dst) in enumerate(((mean_out, mean_hbm), (square_out, square_hbm))):
        copy = pltpu.make_async_copy(src, dst, out_sem.at[2 * rows + i])
        copy.start()
        puts.append(copy)
    for copy in puts:
        copy.wait()


def per_device(
    activations, weight, gamma, beta, group_map, lengths, stale_edges,
    stale_mean, stale_square, old_mean, old_square,
):
    rows, width, local = activations.shape
    channels = weight.shape[1]
    groups = stale_mean.shape[0]
    strips, chans = lax.axis_size("strip"), lax.axis_size("chan")
    ny, nz = torus(strips)
    pairs = rows // 2

    def turned(v):
        return jnp.swapaxes(v, 1, 2)

    dma = pltpu.SemaphoreType.DMA
    any_space = pl.BlockSpec(memory_space=pl.ANY)
    smem = pl.BlockSpec(memory_space=pltpu.SMEM)
    flops = 2 * rows * width * 9 * channels * local
    block, moments = pl.pallas_call(
        functools.partial(main_kernel, rows, width, strips, chans, channels // groups),
        name="gather_conv",
        out_shape=(
            jax.ShapeDtypeStruct((rows, local, width), BF16),
            jax.ShapeDtypeStruct((8, LANES), F32),
        ),
        in_specs=[any_space] * 6 + [smem] + [any_space] * 4,
        out_specs=(any_space, any_space),
        scratch_shapes=[
            pltpu.VMEM((channels // LANES, LANES), F32),
            pltpu.VMEM((channels // LANES, LANES), F32),
            pltpu.VMEM((channels // LANES, LANES), jnp.int32),
            pltpu.VMEM((1, groups), F32),
            pltpu.VMEM((1, groups), F32),
            pltpu.VMEM((1, groups), F32),
            pltpu.VMEM((1, groups), F32),
            pltpu.VMEM((8, LANES), F32),
            dma((8,)),
            pltpu.VMEM((local, width), BF16),
            pltpu.VMEM((chans, rows + 2, local, width), BF16),
            pltpu.VMEM((chans, 3 * MAIN, (rows + 2) * width), BF16),
            pltpu.VMEM((2, 3 * LANES, (rows + 2) * width), BF16),
            pltpu.VMEM((3, chans, local, 3 * MAIN), BF16),
            pltpu.VMEM((3, 2, local, 3 * LANES), BF16),
            pltpu.VMEM((local, rows * width), F32),
            pltpu.VMEM((rows, local, width), BF16),
            pltpu.VMEM((LANES, LANES), F32),
            pltpu.VMEM((channels, LANES), jnp.int32),
            pltpu.VMEM((2, channels, LANES), F32),
            pltpu.VMEM((4, 8, LANES), F32),
            pltpu.VMEM((chans, 8, LANES), F32),
            pltpu.VMEM((2, 8, LANES), F32),
            pltpu.VMEM((nz, 8, LANES), F32),
            pltpu.VMEM((ny, 8, LANES), F32),
            dma((pairs,)),
            dma((chans + 2,)),
            dma((2, pairs + 1)),
            dma((2, pairs + 1)),
            dma((2, 6)),
            dma((2, 6)),
            dma((3,)),
            dma((3,)),
            dma((3 + nz + ny,)),
            dma((chans - 1,)),
            dma((1,)),
            dma((max(nz - 1, 1),)),
            dma((max(ny - 1, 1),)),
            dma((pairs,)),
        ],
        compiler_params=pltpu.CompilerParams(
            collective_id=0, has_side_effects=True, vmem_limit_bytes=60 * 1024 * 1024
        ),
        cost_estimate=pl.CostEstimate(
            flops=flops, bytes_accessed=weight.size * 2, transcendentals=rows * width * channels
        ),
    )(
        turned(activations), turned(stale_edges), turned(weight),
        gamma.reshape(-1, LANES), beta.reshape(-1, LANES), group_map.reshape(-1, LANES), lengths,
        stale_mean.reshape(1, groups), stale_square.reshape(1, groups), old_mean, old_square,
    )

    upsampled, new_mean, new_square = pl.pallas_call(
        functools.partial(spread_kernel, rows, width, local),
        name="spread",
        out_shape=(
            jax.ShapeDtypeStruct((2 * rows, local, 2 * width), BF16),
            jax.ShapeDtypeStruct((1, groups), F32),
            jax.ShapeDtypeStruct((1, groups), F32),
        ),
        in_specs=[any_space, any_space],
        out_specs=(any_space, any_space, any_space),
        scratch_shapes=[
            pltpu.VMEM((rows, local, width), BF16),
            pltpu.VMEM((8, LANES), F32),
            pltpu.VMEM((1, groups), F32),
            pltpu.VMEM((1, groups), F32),
            pltpu.VMEM((rows, local, 2 * width), BF16),
            dma((pairs + 1,)),
            dma((2 * rows + 2,)),
        ],
        compiler_params=pltpu.CompilerParams(vmem_limit_bytes=60 * 1024 * 1024),
    )(block, moments)
    return turned(upsampled), new_mean.reshape(groups), new_square.reshape(groups)


def solution(mesh):
    in_specs = (
        P("strip", None, "chan"),
        P(None, None, "chan"),
        P(),
        P(),
        P(),
        P("strip"),
        P("strip", None, "chan"),
        P(),
        P(),
        P("strip", None),
        P("strip", None),
    )
    out_specs = (P("strip", None, "chan"), P(), P())
    return jax.shard_map(
        per_device, mesh=mesh, in_specs=in_specs, out_specs=out_specs, check_vma=False
    )
```

```python
import functools

import jax
import jax.numpy as jnp
from jax import lax
from jax.experimental import pallas as pl
from jax.experimental.pallas import tpu as pltpu
from jax.sharding import PartitionSpec as P

EPS = 1e-05
F32 = jnp.float32
BF16 = jnp.bfloat16
MAIN = 256
REM = 64
SLAB = MAIN + REM
LANES = 128


def torus(strips):
    return {64: (4, 8), 4: (1, 2)}[strips]


def main_kernel(
    rows, width, strips, chans, per_group,
    act_hbm, edge_hbm, weight_hbm, *rest
):
    (
        gamma_hbm, beta_hbm, groups_hbm, lengths,
        stale_mean_hbm, stale_square_hbm, old_mean_hbm, old_square_hbm,
        block_hbm, moments_hbm,
        gamma, beta, groups_of, stale_mean, stale_square, old_mean, old_square, moments,
        small_sem, hop, raw, feats, feats_rem, wts, wts_rem, acc, block, columns, group_col, affine,
    st_own, st_chan, st_core, st_z, st_y,
    load_sem, wt_sem, own_send, own_recv, fwd_send, fwd_recv, edge_send, edge_recv,
    stat_send, chan_recv, core_recv, z_recv, y_recv, out_sem,
    ) = rest
    ny, nz = torus(strips)
    pairs = rows // 2
    tiles = chans * SLAB // LANES
    x = lax.axis_index("chan")
    s = lax.axis_index("strip")
    core = s % 2
    z = (s // 2) % nz
    y = s // (2 * nz)
    right, left, far = (x + 1) % chans, (x + 3) % chans, (x + 2) % chans
    partner = s + 1 - 2 * core
    z_peer = (y * nz + (z + 2 * core + nz - 1) % nz) * 2 + 1 - core
    turns = z == core * (nz - 1)
    peer_turns = (z + 2 * core + nz - 1) % nz == (1 - core) * (nz - 1)
    slabs = (x, left, right, far)

    def slab_of(j):
        return (x + (j % 2) * ((7 - j) // 2) + (1 - j % 2) * (j // 2)) % chans

    def to_z(k):
        return (y * nz + (z + k) % nz) * 2 + core

    def to_y(k):
        return (((y + k) % ny) * nz + z) * 2 + core

    loads = []
    for c in range(pairs):
        copy = pltpu.make_async_copy(
            act_hbm.at[pl.ds(2 * c, 2)], raw.at[0, pl.ds(2 * c, 2)], load_sem.at[c]
        )
        copy.start()
        loads.append(copy)

    small = []
    for i, (src, dst) in enumerate(
        (
            (gamma_hbm, gamma), (beta_hbm, beta), (groups_hbm, groups_of),
            (stale_mean_hbm, stale_mean), (stale_square_hbm, stale_square),
            (old_mean_hbm, old_mean), (old_square_hbm, old_square),
        )
    ):
        copy = pltpu.make_async_copy(src, dst, small_sem.at[i])
        copy.start()
        small.append(copy)

    barrier = pltpu.get_barrier_semaphore()
    greeted = 0
    for target in (right, left, far):
        pl.semaphore_signal(barrier, inc=1, device_id={"chan": target})
        greeted += 1
    others = [partner, z_peer] + [to_y(k) for k in range(1, ny)]
    for target in others:
        pl.semaphore_signal(barrier, inc=1, device_id={"strip": target})
        greeted += 1

    def main_start(slab):
        return pl.multiple_of(SLAB * slab + REM * (slab % 2), LANES)

    for j in range(chans):
        for dy in range(3):
            for dx in range(3):
                pltpu.make_async_copy(
                    weight_hbm.at[3 * dy + dx, :, pl.ds(main_start(slabs[j]), MAIN)],
                    wts.at[dy, j, :, pl.ds(dx * MAIN, MAIN)],
                    wt_sem.at[j],
                ).start()
    for g in range(2):
        first = pl.multiple_of(MAIN + 2 * SLAB * ((x // 2 + g) % 2), LANES)
        for dy in range(3):
            for dx in range(3):
                pltpu.make_async_copy(
                    weight_hbm.at[3 * dy + dx, :, pl.ds(first, LANES)],
                    wts_rem.at[dy, g, :, pl.ds(dx * LANES, LANES)],
                    wt_sem.at[chans + g],
                ).start()

    lane = lax.broadcasted_iota(jnp.int32, (1, LANES), 1)
    length = jnp.full((1, LANES), lengths[0], jnp.int32)

    for copy in small:
        copy.wait()
    columns[...] = jnp.transpose(
        jnp.concatenate(
            [
                gamma[...], beta[...], groups_of[...].astype(F32),
                jnp.zeros((LANES - 3 * tiles, LANES), F32),
            ],
            axis=0,
        )
    )
    for t in range(tiles):
        group_col[t * LANES:(t + 1) * LANES] = jnp.broadcast_to(
            columns[:, 2 * tiles + t:2 * tiles + t + 1], (LANES, LANES)
        ).astype(jnp.int32)

    pl.semaphore_wait(barrier, greeted)

    sends = []

    def send(src, dst, send_sem, recv_sem, target):
        copy = pltpu.make_async_remote_copy(
            src_ref=src, dst_ref=dst, send_sem=send_sem, recv_sem=recv_sem,
            device_id=target, device_id_type=pl.DeviceIdType.MESH,
        )
        copy.start()
        sends.append(copy)

    def wait_for(dst, sem):
        pltpu.make_async_copy(dst, dst, sem).wait()

    edge = pairs

    def pair_of(j, c):
        return raw.at[j, pl.ds(2 * c, 2)]

    def send_own(c):
        for d, target in enumerate((right, left)):
            send(
                pair_of(0, c), pair_of(1 + d, c), own_send.at[d, c], own_recv.at[d, c],
                {"chan": target},
            )

    for copy in loads:
        copy.wait()
    send_own(0)
    send(
        edge_hbm.at[1 - core], raw.at[0, rows + core], edge_send.at[0], edge_recv.at[0],
        {"strip": partner},
    )

    @pl.when(peer_turns)
    def _():
        pltpu.make_async_remote_copy(
            src_ref=edge_hbm.at[core], dst_ref=hop, send_sem=edge_send.at[1],
            recv_sem=edge_recv.at[1], device_id={"strip": z_peer},
            device_id_type=pl.DeviceIdType.MESH,
        ).start()

    @pl.when(jnp.logical_not(peer_turns))
    def _():
        pltpu.make_async_remote_copy(
            src_ref=edge_hbm.at[core], dst_ref=raw.at[0, rows + 1 - core],
            send_sem=edge_send.at[1], recv_sem=edge_recv.at[1], device_id={"strip": z_peer},
            device_id_type=pl.DeviceIdType.MESH,
        ).start()

    group_one = jnp.zeros((1, LANES), F32)
    group_two = jnp.zeros((1, LANES), F32)
    for i in range(SLAB // REM):
        one = jnp.zeros((REM, LANES), F32)
        two = jnp.zeros((REM, LANES), F32)
        for q in range(rows):
            v = jnp.where(q < length, raw[0, q, i * REM:(i + 1) * REM, :].astype(F32), 0.0)
            one = one + v
            two = two + v * v
        own_at = pl.ds(pl.multiple_of(SLAB * x + REM * i, REM), REM)
        member = group_col[own_at] == lane
        chan_one = jnp.sum(one, axis=1, keepdims=True)
        chan_two = jnp.sum(two, axis=1, keepdims=True)
        group_one = group_one + jnp.sum(jnp.where(member, chan_one, 0.0), axis=0, keepdims=True)
        group_two = group_two + jnp.sum(jnp.where(member, chan_two, 0.0), axis=0, keepdims=True)
    own = jnp.concatenate([group_one, group_two, jnp.zeros((6, LANES), F32)], axis=0)
    st_own[0] = own
    st_chan[x] = own
    for k in range(1, chans):
        send(
            st_own.at[0], st_chan.at[x], stat_send.at[k - 1], chan_recv.at[k - 1],
            {"chan": (x + k) % chans},
        )
    send_own(1)
    wait_for(raw.at[0, rows + 1 - core], edge_recv.at[0])

    @pl.when(turns)
    def _():
        wait_for(hop, edge_recv.at[1])
        pltpu.make_async_remote_copy(
            src_ref=hop, dst_ref=raw.at[0, rows + core], send_sem=edge_send.at[2],
            recv_sem=edge_recv.at[2],
            device_id={"strip": ((y + 1 + core * (ny - 2)) % ny * nz + z) * 2 + core},
            device_id_type=pl.DeviceIdType.MESH,
        ).start()
        wait_for(raw.at[0, rows + core], edge_recv.at[2])

    @pl.when(jnp.logical_not(turns))
    def _():
        wait_for(raw.at[0, rows + core], edge_recv.at[1])

    send_own(edge)
    send_own(2)
    send_own(3)

    for k in range(1, chans):
        wait_for(st_chan.at[(x + chans - k) % chans], chan_recv.at[k - 1])
    strip_sum = st_chan[0]
    for k in range(1, chans):
        strip_sum = strip_sum + st_chan[k]
    st_own[1] = strip_sum
    st_core[core] = strip_sum
    groups = stale_mean.shape[1]

    def padded(ref):
        return jnp.concatenate([ref[...], jnp.zeros((1, LANES - groups), F32)], axis=1)

    count = length.astype(F32) * float(width * per_group)
    fresh_mean = strip_sum[0:1] / count
    fresh_square = strip_sum[1:2] / count
    mean = padded(stale_mean) + fresh_mean - padded(old_mean)
    square = padded(stale_square) + fresh_square - padded(old_square)
    var = jnp.maximum(square - mean * mean, 0.5 * (fresh_square - fresh_mean * fresh_mean))
    rstd = lax.rsqrt(var + EPS)
    for t in range(tiles):
        if t == 2:
            send(
                st_own.at[1], st_core.at[core], stat_send.at[3], core_recv.at[0],
                {"strip": partner},
            )
        at = slice(t * LANES, (t + 1) * LANES)
        member = group_col[at] == lane
        rstd_c = jnp.sum(jnp.where(member, rstd, 0.0), axis=1, keepdims=True)
        mean_c = jnp.sum(jnp.where(member, mean, 0.0), axis=1, keepdims=True)
        scale = rstd_c * columns[:, t:t + 1]
        shift = columns[:, tiles + t:tiles + t + 1] - mean_c * scale
        affine[0, at] = jnp.broadcast_to(0.5 * scale, (LANES, LANES))
        affine[1, at] = jnp.broadcast_to(0.5 * shift, (LANES, LANES))

    def flag(condition):
        return jnp.where(condition, 1.0, 0.0).astype(BF16)

    not_first = flag(lane != 0)
    not_last = flag(lane != width - 1)
    top = flag(jnp.full((1, LANES), s, jnp.int32) > 0)
    bottom = jnp.full((1, LANES), s, jnp.int32) < strips - 1

    def store(j, i, p, a):
        before = pltpu.roll(a, 1, 1) * not_first
        after = pltpu.roll(a, width - 1, 1) * not_last
        cells = pl.ds(pl.multiple_of(p * width, LANES), width)
        if i < MAIN // REM:
            for dx, v in enumerate((before, a, after)):
                feats[j, dx * MAIN + i * REM:dx * MAIN + (i + 1) * REM, cells] = v
        else:
            slab = slab_of(j)
            g = (slab // 2 + x // 2) % 2
            for dx, v in enumerate((before, a, after)):
                at = pl.ds(pl.multiple_of(dx * LANES + REM * (slab % 2), REM), REM)
                feats_rem[g, at, cells] = v

    def piece(j, i):
        odd = slab_of(j) % 2
        if i < MAIN // REM:
            return REM * i + REM * odd
        return MAIN * (1 - odd)

    def at_piece(start):
        return pl.ds(pl.multiple_of(start, REM), REM)

    def prepare(j, q):
        row = jnp.zeros((1, LANES), jnp.int32) + q
        in_use = flag(row < length)
        border = flag((row == length) & bottom)
        for i in range(SLAB // REM):
            start = piece(j, i)
            total = at_piece(SLAB * slab_of(j) + start)
            h = raw[j, q, at_piece(start), :].astype(F32) * affine[0, total] + affine[1, total]
            a = (h + h * jnp.tanh(h)).astype(BF16)
            store(j, i, q + 1, a * in_use + raw[j, rows + 1, at_piece(start), :] * border)

    def prepare_edge(j):
        border = flag((length == rows) & bottom)
        for i in range(SLAB // REM):
            start = piece(j, i)
            store(j, i, 0, raw[j, rows, at_piece(start), :] * top)
            store(j, i, rows + 1, raw[j, rows + 1, at_piece(start), :] * border)

    def prepare_pair(j, c):
        prepare(j, 2 * c)
        prepare(j, 2 * c + 1)

    def cells_of(pair, dy):
        return pl.ds(pl.multiple_of((2 * pair + dy) * width, LANES), 2 * width)

    def term(j, pair, dy):
        return jnp.dot(wts[dy, j], feats[j, :, cells_of(pair, dy)], preferred_element_type=F32)

    def term_rem(g, pair, dy):
        return jnp.dot(
            wts_rem[dy, g], feats_rem[g, :, cells_of(pair, dy)], preferred_element_type=F32
        )

    def add_to(pair, total, first=False):
        at = pl.ds(pl.multiple_of(pair * 2 * width, LANES), 2 * width)
        acc[:, at] = total if first else acc[:, at] + total

    def products(pair, steps, slabs_in, groups_in):
        total = None
        for dy in steps:
            for j in slabs_in:
                one = term(j, pair, dy)
                total = one if total is None else total + one
            for g in groups_in:
                total = total + term_rem(g, pair, dy)
        return total

    def wait_weights(j):
        pltpu.make_async_copy(wts.at[:, j], wts.at[:, j], wt_sem.at[j]).wait()

    def wait_weights_rem(g):
        pltpu.make_async_copy(wts_rem.at[:, g], wts_rem.at[:, g], wt_sem.at[chans + g]).wait()

    wait_for(st_core.at[1 - core], core_recv.at[0])
    chip_sum = st_core[0] + st_core[1]
    st_own[2] = chip_sum
    st_z[z] = chip_sum

    reach = ((1, nz - 1), (2, nz - 2), tuple(range(3, nz - 2)))
    if nz < 4:
        reach = ((1,), (), ())

    def send_z(step):
        for k in reach[step]:
            send(
                st_own.at[2], st_z.at[z], stat_send.at[3 + k], z_recv.at[k - 1],
                {"strip": to_z(k)},
            )

    def got_z(step):
        for k in reach[step]:
            wait_for(st_z.at[(z + nz - k) % nz], z_recv.at[k - 1])

    prepare_edge(0)
    send_z(0)

    @pl.loop(0, rows)
    def _(q):
        prepare(0, q)

    wait_weights(0)

    for pair in range(pairs):
        add_to(pair, products(pair, (0, 1, 2), (0,), ()), first=True)


    def got(c):
        for d in range(2):
            wait_for(pair_of(1 + d, c), own_recv.at[d, c])

    plan = [
        [(rows + 1 - d, 0, SLAB)]
        + [(2 * i + d, 0, SLAB) for i in range(pairs - 1)]
        + [(rows - 2, d * (SLAB // 2), SLAB // 2), (rows - 1, d * (SLAB // 2), SLAB // 2)]
        for d in range(2)
    ]

    def forward(d, k):
        q, start, number = plan[d][k]
        part = pl.ds(start, number)
        send(
            raw.at[1 + d, q, part], raw.at[3, q, part], fwd_send.at[d, k], fwd_recv.at[d, k],
            {"chan": (right, left)[d]},
        )

    def got_far(k):
        for d in range(2):
            q, start, number = plan[d][k]
            wait_for(raw.at[3, q, pl.ds(start, number)], fwd_recv.at[d, k])

    got(0)
    got(1)
    got(edge)
    for k in range(3):
        for d in range(2):
            forward(d, k)
    got_z(0)
    send_z(1)
    wait_weights(1)
    wait_weights(2)
    wait_weights_rem(0)

    @pl.loop(1, 3)
    def _(j):
        prepare_edge(j)
        prepare_pair(j, 0)
        prepare_pair(j, 1)

    def add_sides(pair, *steps):
        add_to(pair, products(pair, steps, (1, 2), (0,)))

    add_sides(0, 0, 1, 2)
    add_sides(1, 0, 1)
    got(2)
    for d in range(2):
        forward(d, 3)

    @pl.loop(1, 3)
    def _(j):
        prepare_pair(j, 2)

    add_sides(1, 2)
    add_sides(2, 0, 1)
    got_z(1)
    send_z(2)
    got(3)
    for k in range(4, 6):
        for d in range(2):
            forward(d, k)
    @pl.loop(1, 3)
    def _(j):
        prepare_pair(j, 3)

    add_sides(2, 2)
    add_sides(3, 0, 1, 2)

    wait_weights(3)
    wait_weights_rem(1)
    outs = []

    def finish(pair):
        for h in range(2):
            r = 2 * pair + h
            value = raw[0, r].astype(F32) + acc[:, r * width:(r + 1) * width]
            block[r] = jnp.where(r < length, value, 0.0).astype(BF16)

    def put(pair):
        at = pl.ds(2 * pair, 2)
        copy = pltpu.make_async_copy(block.at[at], block_hbm.at[at], out_sem.at[pair])
        copy.start()
        outs.append(copy)

    def both(pair, *steps):
        add_to(pair, products(pair, steps, (3,), (1,)))

    got_far(0)
    prepare_edge(3)
    got_far(1)
    prepare_pair(3, 0)
    both(0, 0, 1)
    got_z(2)
    line_sum = st_z[0]
    for k in range(1, nz):
        line_sum = line_sum + st_z[k]
    st_own[3] = line_sum
    st_y[y] = line_sum

    got_far(2)
    prepare_pair(3, 1)
    for k in range(1, ny):
        send(
            st_own.at[3], st_y.at[y], stat_send.at[2 + nz + k], y_recv.at[k - 1],
            {"strip": to_y(k)},
        )
    both(0, 2)
    finish(0)
    both(1, 0, 1)
    put(0)
    got_far(3)
    prepare_pair(3, 2)
    both(1, 2)
    finish(1)
    both(2, 0, 1)
    put(1)
    got_far(4)
    prepare(3, rows - 2)
    both(2, 2)
    finish(2)
    both(3, 0)
    put(2)
    got_far(5)
    prepare(3, rows - 1)
    both(3, 1, 2)
    finish(3)
    put(3)

    for k in range(1, ny):
        wait_for(st_y.at[(y + ny - k) % ny], y_recv.at[k - 1])
    image_sum = st_y[0]
    for k in range(1, ny):
        image_sum = image_sum + st_y[k]
    moments[...] = image_sum / float(strips * (3 * rows // 4) * width * per_group)
    copy = pltpu.make_async_copy(moments, moments_hbm, small_sem.at[7])
    copy.start()
    outs.append(copy)
    for copy in sends:
        copy.wait_send()
    wait_for(edge_hbm.at[0], edge_send.at[1])

    @pl.when(turns)
    def _():
        wait_for(hop, edge_send.at[2])

    for copy in outs:
        copy.wait()


def spread_kernel(
    rows, width, local, block_hbm, moments_hbm, up_hbm, mean_hbm, square_hbm,
    block, moments, mean_out, square_out, buf, in_sem, out_sem,
):
    takes = []
    for r in range(0, rows, 2):
        at = pl.ds(r, 2)
        copy = pltpu.make_async_copy(block_hbm.at[at], block.at[at], in_sem.at[r // 2])
        copy.start()
        takes.append(copy)
    take = pltpu.make_async_copy(moments_hbm, moments, in_sem.at[rows // 2])
    take.start()
    twice = (
        lax.broadcasted_iota(jnp.int32, (width, 2 * width), 1) // 2
        == lax.broadcasted_iota(jnp.int32, (width, 2 * width), 0)
    ).astype(F32).astype(BF16)
    puts = []
    for r in range(rows):
        if r % 2 == 0:
            takes[r // 2].wait()
        buf[r] = jnp.dot(block[r], twice, preferred_element_type=F32).astype(BF16)
        for a in range(2):
            copy = pltpu.make_async_copy(buf.at[r], up_hbm.at[2 * r + a], out_sem.at[2 * r + a])
            copy.start()
            puts.append(copy)
    groups = mean_out.shape[1]
    take.wait()
    mean_out[...] = moments[0:1, 0:groups]
    square_out[...] = moments[1:2, 0:groups]
    for i, (src, dst) in enumerate(((mean_out, mean_hbm), (square_out, square_hbm))):
        copy = pltpu.make_async_copy(src, dst, out_sem.at[2 * rows + i])
        copy.start()
        puts.append(copy)
    for copy in puts:
        copy.wait()


def per_device(
    activations, weight, gamma, beta, group_map, lengths, stale_edges,
    stale_mean, stale_square, old_mean, old_square,
):
    rows, width, local = activations.shape
    channels = weight.shape[1]
    groups = stale_mean.shape[0]
    strips, chans = lax.axis_size("strip"), lax.axis_size("chan")
    ny, nz = torus(strips)
    pairs = rows // 2

    def turned(v):
        return jnp.swapaxes(v, 1, 2)

    dma = pltpu.SemaphoreType.DMA
    any_space = pl.BlockSpec(memory_space=pl.ANY)
    smem = pl.BlockSpec(memory_space=pltpu.SMEM)
    flops = 2 * rows * width * 9 * channels * local
    block, moments = pl.pallas_call(
        functools.partial(main_kernel, rows, width, strips, chans, channels // groups),
        name="gather_conv",
        out_shape=(
            jax.ShapeDtypeStruct((rows, local, width), BF16),
            jax.ShapeDtypeStruct((8, LANES), F32),
        ),
        in_specs=[any_space] * 6 + [smem] + [any_space] * 4,
        out_specs=(any_space, any_space),
        scratch_shapes=[
            pltpu.VMEM((channels // LANES, LANES), F32),
            pltpu.VMEM((channels // LANES, LANES), F32),
            pltpu.VMEM((channels // LANES, LANES), jnp.int32),
            pltpu.VMEM((1, groups), F32),
            pltpu.VMEM((1, groups), F32),
            pltpu.VMEM((1, groups), F32),
            pltpu.VMEM((1, groups), F32),
            pltpu.VMEM((8, LANES), F32),
            dma((8,)),
            pltpu.VMEM((local, width), BF16),
            pltpu.VMEM((chans, rows + 2, local, width), BF16),
            pltpu.VMEM((chans, 3 * MAIN, (rows + 2) * width), BF16),
            pltpu.VMEM((2, 3 * LANES, (rows + 2) * width), BF16),
            pltpu.VMEM((3, chans, local, 3 * MAIN), BF16),
            pltpu.VMEM((3, 2, local, 3 * LANES), BF16),
            pltpu.VMEM((local, rows * width), F32),
            pltpu.VMEM((rows, local, width), BF16),
            pltpu.VMEM((LANES, LANES), F32),
            pltpu.VMEM((channels, LANES), jnp.int32),
            pltpu.VMEM((2, channels, LANES), F32),
            pltpu.VMEM((4, 8, LANES), F32),
            pltpu.VMEM((chans, 8, LANES), F32),
            pltpu.VMEM((2, 8, LANES), F32),
            pltpu.VMEM((nz, 8, LANES), F32),
            pltpu.VMEM((ny, 8, LANES), F32),
            dma((pairs,)),
            dma((chans + 2,)),
            dma((2, pairs + 1)),
            dma((2, pairs + 1)),
            dma((2, 6)),
            dma((2, 6)),
            dma((3,)),
            dma((3,)),
            dma((3 + nz + ny,)),
            dma((chans - 1,)),
            dma((1,)),
            dma((max(nz - 1, 1),)),
            dma((max(ny - 1, 1),)),
            dma((pairs,)),
        ],
        compiler_params=pltpu.CompilerParams(
            collective_id=0, has_side_effects=True, vmem_limit_bytes=60 * 1024 * 1024
        ),
        cost_estimate=pl.CostEstimate(
            flops=flops, bytes_accessed=weight.size * 2, transcendentals=rows * width * channels
        ),
    )(
        turned(activations), turned(stale_edges), turned(weight),
        gamma.reshape(-1, LANES), beta.reshape(-1, LANES), group_map.reshape(-1, LANES), lengths,
        stale_mean.reshape(1, groups), stale_square.reshape(1, groups), old_mean, old_square,
    )

    upsampled, new_mean, new_square = pl.pallas_call(
        functools.partial(spread_kernel, rows, width, local),
        name="spread",
        out_shape=(
            jax.ShapeDtypeStruct((2 * rows, local, 2 * width), BF16),
            jax.ShapeDtypeStruct((1, groups), F32),
            jax.ShapeDtypeStruct((1, groups), F32),
        ),
        in_specs=[any_space, any_space],
        out_specs=(any_space, any_space, any_space),
        scratch_shapes=[
            pltpu.VMEM((rows, local, width), BF16),
            pltpu.VMEM((8, LANES), F32),
            pltpu.VMEM((1, groups), F32),
            pltpu.VMEM((1, groups), F32),
            pltpu.VMEM((rows, local, 2 * width), BF16),
            dma((pairs + 1,)),
            dma((2 * rows + 2,)),
        ],
        compiler_params=pltpu.CompilerParams(vmem_limit_bytes=60 * 1024 * 1024),
    )(block, moments)
    return turned(upsampled), new_mean.reshape(groups), new_square.reshape(groups)


def solution(mesh):
    in_specs = (
        P("strip", None, "chan"),
        P(None, None, "chan"),
        P(),
        P(),
        P(),
        P("strip"),
        P("strip", None, "chan"),
        P(),
        P(),
        P("strip", None),
        P("strip", None),
    )
    out_specs = (P("strip", None, "chan"), P(), P())
    return jax.shard_map(
        per_device, mesh=mesh, in_specs=in_specs, out_specs=out_specs, check_vma=False
    )
```

```python
import functools

import jax
import jax.numpy as jnp
from jax import lax
from jax.experimental import pallas as pl
from jax.experimental.pallas import tpu as pltpu
from jax.sharding import PartitionSpec as P

EPS = 1e-05
F32 = jnp.float32
BF16 = jnp.bfloat16
MAIN = 256
REM = 64
SLAB = MAIN + REM
LANES = 128


def torus(strips):
    return {64: (4, 8), 4: (1, 2)}[strips]


def main_kernel(
    rows, width, strips, chans, per_group,
    act_hbm, edge_hbm, weight_hbm, *rest
):
    (
        gamma_hbm, beta_hbm, groups_hbm, lengths,
        stale_mean_hbm, stale_square_hbm, old_mean_hbm, old_square_hbm,
        block_hbm, moments_hbm,
        gamma, beta, groups_of, stale_mean, stale_square, old_mean, old_square, moments,
        small_sem, hop, raw, feats, feats_rem, wts, wts_rem, acc, block, columns, group_col, affine,
    st_own, st_chan, st_core, st_z, st_y,
    load_sem, wt_sem, own_send, own_recv, fwd_send, fwd_recv, edge_send, edge_recv,
    stat_send, chan_recv, core_recv, z_recv, y_recv, out_sem,
    ) = rest
    ny, nz = torus(strips)
    pairs = rows // 2
    tiles = chans * SLAB // LANES
    x = lax.axis_index("chan")
    s = lax.axis_index("strip")
    core = s % 2
    z = (s // 2) % nz
    y = s // (2 * nz)
    right, left, far = (x + 1) % chans, (x + 3) % chans, (x + 2) % chans
    partner = s + 1 - 2 * core
    z_peer = (y * nz + (z + 2 * core + nz - 1) % nz) * 2 + 1 - core
    turns = z == core * (nz - 1)
    peer_turns = (z + 2 * core + nz - 1) % nz == (1 - core) * (nz - 1)
    slabs = (x, left, right, far)

    def slab_of(j):
        return (x + (j % 2) * ((7 - j) // 2) + (1 - j % 2) * (j // 2)) % chans

    def to_z(k):
        return (y * nz + (z + k) % nz) * 2 + core

    def to_y(k):
        return (((y + k) % ny) * nz + z) * 2 + core

    loads = []
    for c in range(pairs):
        copy = pltpu.make_async_copy(
            act_hbm.at[pl.ds(2 * c, 2)], raw.at[0, pl.ds(2 * c, 2)], load_sem.at[c]
        )
        copy.start()
        loads.append(copy)

    small = []
    for i, (src, dst) in enumerate(
        (
            (gamma_hbm, gamma), (beta_hbm, beta), (groups_hbm, groups_of),
            (stale_mean_hbm, stale_mean), (stale_square_hbm, stale_square),
            (old_mean_hbm, old_mean), (old_square_hbm, old_square),
        )
    ):
        copy = pltpu.make_async_copy(src, dst, small_sem.at[i])
        copy.start()
        small.append(copy)

    barrier = pltpu.get_barrier_semaphore()
    greeted = 0
    for target in (right, left, far):
        pl.semaphore_signal(barrier, inc=1, device_id={"chan": target})
        greeted += 1
    others = [partner, z_peer] + [to_y(k) for k in range(1, ny)]
    for target in others:
        pl.semaphore_signal(barrier, inc=1, device_id={"strip": target})
        greeted += 1

    def main_start(slab):
        return pl.multiple_of(SLAB * slab + REM * (slab % 2), LANES)

    for j in range(chans):
        for dy in range(3):
            for dx in range(3):
                pltpu.make_async_copy(
                    weight_hbm.at[3 * dy + dx, :, pl.ds(main_start(slabs[j]), MAIN)],
                    wts.at[dy, j, :, pl.ds(dx * MAIN, MAIN)],
                    wt_sem.at[j],
                ).start()
    for g in range(2):
        first = pl.multiple_of(MAIN + 2 * SLAB * ((x // 2 + g) % 2), LANES)
        for dy in range(3):
            for dx in range(3):
                pltpu.make_async_copy(
                    weight_hbm.at[3 * dy + dx, :, pl.ds(first, LANES)],
                    wts_rem.at[dy, g, :, pl.ds(dx * LANES, LANES)],
                    wt_sem.at[chans + g],
                ).start()

    lane = lax.broadcasted_iota(jnp.int32, (1, LANES), 1)
    length = jnp.full((1, LANES), lengths[0], jnp.int32)

    for copy in small:
        copy.wait()
    columns[...] = jnp.transpose(
        jnp.concatenate(
            [
                gamma[...], beta[...], groups_of[...].astype(F32),
                jnp.zeros((LANES - 3 * tiles, LANES), F32),
            ],
            axis=0,
        )
    )
    for t in range(tiles):
        group_col[t * LANES:(t + 1) * LANES] = jnp.broadcast_to(
            columns[:, 2 * tiles + t:2 * tiles + t + 1], (LANES, LANES)
        ).astype(jnp.int32)

    pl.semaphore_wait(barrier, greeted)

    sends = []

    def send(src, dst, send_sem, recv_sem, target):
        copy = pltpu.make_async_remote_copy(
            src_ref=src, dst_ref=dst, send_sem=send_sem, recv_sem=recv_sem,
            device_id=target, device_id_type=pl.DeviceIdType.MESH,
        )
        copy.start()
        sends.append(copy)

    def wait_for(dst, sem):
        pltpu.make_async_copy(dst, dst, sem).wait()

    edge = pairs

    def pair_of(j, c):
        return raw.at[j, pl.ds(2 * c, 2)]

    def send_own(c):
        for d, target in enumerate((right, left)):
            send(
                pair_of(0, c), pair_of(1 + d, c), own_send.at[d, c], own_recv.at[d, c],
                {"chan": target},
            )

    for copy in loads:
        copy.wait()
    send_own(0)
    send(
        edge_hbm.at[1 - core], raw.at[0, rows + core], edge_send.at[0], edge_recv.at[0],
        {"strip": partner},
    )

    @pl.when(peer_turns)
    def _():
        pltpu.make_async_remote_copy(
            src_ref=edge_hbm.at[core], dst_ref=hop, send_sem=edge_send.at[1],
            recv_sem=edge_recv.at[1], device_id={"strip": z_peer},
            device_id_type=pl.DeviceIdType.MESH,
        ).start()

    @pl.when(jnp.logical_not(peer_turns))
    def _():
        pltpu.make_async_remote_copy(
            src_ref=edge_hbm.at[core], dst_ref=raw.at[0, rows + 1 - core],
            send_sem=edge_send.at[1], recv_sem=edge_recv.at[1], device_id={"strip": z_peer},
            device_id_type=pl.DeviceIdType.MESH,
        ).start()

    group_one = jnp.zeros((1, LANES), F32)
    group_two = jnp.zeros((1, LANES), F32)
    for i in range(SLAB // REM):
        one = jnp.zeros((REM, LANES), F32)
        two = jnp.zeros((REM, LANES), F32)
        for q in range(rows):
            v = jnp.where(q < length, raw[0, q, i * REM:(i + 1) * REM, :].astype(F32), 0.0)
            one = one + v
            two = two + v * v
        own_at = pl.ds(pl.multiple_of(SLAB * x + REM * i, REM), REM)
        member = group_col[own_at] == lane
        chan_one = jnp.sum(one, axis=1, keepdims=True)
        chan_two = jnp.sum(two, axis=1, keepdims=True)
        group_one = group_one + jnp.sum(jnp.where(member, chan_one, 0.0), axis=0, keepdims=True)
        group_two = group_two + jnp.sum(jnp.where(member, chan_two, 0.0), axis=0, keepdims=True)
    own = jnp.concatenate([group_one, group_two, jnp.zeros((6, LANES), F32)], axis=0)
    st_own[0] = own
    st_chan[x] = own
    for k in range(1, chans):
        send(
            st_own.at[0], st_chan.at[x], stat_send.at[k - 1], chan_recv.at[k - 1],
            {"chan": (x + k) % chans},
        )
    send_own(1)
    wait_for(raw.at[0, rows + 1 - core], edge_recv.at[0])

    @pl.when(turns)
    def _():
        wait_for(hop, edge_recv.at[1])
        pltpu.make_async_remote_copy(
            src_ref=hop, dst_ref=raw.at[0, rows + core], send_sem=edge_send.at[2],
            recv_sem=edge_recv.at[2],
            device_id={"strip": ((y + 1 + core * (ny - 2)) % ny * nz + z) * 2 + core},
            device_id_type=pl.DeviceIdType.MESH,
        ).start()
        wait_for(raw.at[0, rows + core], edge_recv.at[2])

    @pl.when(jnp.logical_not(turns))
    def _():
        wait_for(raw.at[0, rows + core], edge_recv.at[1])

    send_own(edge)
    send_own(2)
    send_own(3)

    for k in range(1, chans):
        wait_for(st_chan.at[(x + chans - k) % chans], chan_recv.at[k - 1])
    strip_sum = st_chan[0]
    for k in range(1, chans):
        strip_sum = strip_sum + st_chan[k]
    st_own[1] = strip_sum
    st_core[core] = strip_sum
    groups = stale_mean.shape[1]

    def padded(ref):
        return jnp.concatenate([ref[...], jnp.zeros((1, LANES - groups), F32)], axis=1)

    count = length.astype(F32) * float(width * per_group)
    fresh_mean = strip_sum[0:1] / count
    fresh_square = strip_sum[1:2] / count
    mean = padded(stale_mean) + fresh_mean - padded(old_mean)
    square = padded(stale_square) + fresh_square - padded(old_square)
    var = jnp.maximum(square - mean * mean, 0.5 * (fresh_square - fresh_mean * fresh_mean))
    rstd = lax.rsqrt(var + EPS)
    for t in range(tiles):
        if t == 2:
            send(
                st_own.at[1], st_core.at[core], stat_send.at[3], core_recv.at[0],
                {"strip": partner},
            )
        at = slice(t * LANES, (t + 1) * LANES)
        member = group_col[at] == lane
        rstd_c = jnp.sum(jnp.where(member, rstd, 0.0), axis=1, keepdims=True)
        mean_c = jnp.sum(jnp.where(member, mean, 0.0), axis=1, keepdims=True)
        scale = rstd_c * columns[:, t:t + 1]
        shift = columns[:, tiles + t:tiles + t + 1] - mean_c * scale
        affine[0, at] = jnp.broadcast_to(0.5 * scale, (LANES, LANES))
        affine[1, at] = jnp.broadcast_to(0.5 * shift, (LANES, LANES))

    def flag(condition):
        return jnp.where(condition, 1.0, 0.0).astype(BF16)

    not_first = flag(lane != 0)
    not_last = flag(lane != width - 1)
    top = flag(jnp.full((1, LANES), s, jnp.int32) > 0)
    bottom = jnp.full((1, LANES), s, jnp.int32) < strips - 1

    def store(j, i, p, a):
        before = pltpu.roll(a, 1, 1) * not_first
        after = pltpu.roll(a, width - 1, 1) * not_last
        cells = pl.ds(pl.multiple_of(p * width, LANES), width)
        if i < MAIN // REM:
            for dx, v in enumerate((before, a, after)):
                feats[j, dx * MAIN + i * REM:dx * MAIN + (i + 1) * REM, cells] = v
        else:
            slab = slab_of(j)
            g = (slab // 2 + x // 2) % 2
            for dx, v in enumerate((before, a, after)):
                at = pl.ds(pl.multiple_of(dx * LANES + REM * (slab % 2), REM), REM)
                feats_rem[g, at, cells] = v

    def piece(j, i):
        odd = slab_of(j) % 2
        if i < MAIN // REM:
            return REM * i + REM * odd
        return MAIN * (1 - odd)

    def at_piece(start):
        return pl.ds(pl.multiple_of(start, REM), REM)

    def prepare(j, q):
        row = jnp.zeros((1, LANES), jnp.int32) + q
        in_use = flag(row < length)
        border = flag((row == length) & bottom)
        for i in range(SLAB // REM):
            start = piece(j, i)
            total = at_piece(SLAB * slab_of(j) + start)
            h = raw[j, q, at_piece(start), :].astype(F32) * affine[0, total] + affine[1, total]
            a = (h + h * jnp.tanh(h)).astype(BF16)
            store(j, i, q + 1, a * in_use + raw[j, rows + 1, at_piece(start), :] * border)

    def prepare_edge(j):
        border = flag((length == rows) & bottom)
        for i in range(SLAB // REM):
            start = piece(j, i)
            store(j, i, 0, raw[j, rows, at_piece(start), :] * top)
            store(j, i, rows + 1, raw[j, rows + 1, at_piece(start), :] * border)

    def prepare_pair(j, c):
        prepare(j, 2 * c)
        prepare(j, 2 * c + 1)

    def cells_of(pair, dy):
        return pl.ds(pl.multiple_of((2 * pair + dy) * width, LANES), 2 * width)

    def term(j, pair, dy):
        return jnp.dot(wts[dy, j], feats[j, :, cells_of(pair, dy)], preferred_element_type=F32)

    def add_to(pair, total, first=False):
        at = pl.ds(pl.multiple_of(pair * 2 * width, LANES), 2 * width)
        acc[:, at] = total if first else acc[:, at] + total

    def term_rems(g, pair, steps):
        left_side = jnp.concatenate([wts_rem[dy, g] for dy in steps], axis=1)
        patch = jnp.concatenate([feats_rem[g, :, cells_of(pair, dy)] for dy in steps], axis=0)
        return jnp.dot(left_side, patch, preferred_element_type=F32)

    def products(pair, steps, slabs_in, groups_in):
        total = None
        for j in slabs_in:
            for dy in steps:
                one = term(j, pair, dy)
                total = one if total is None else total + one
        for g in groups_in:
            total = total + term_rems(g, pair, steps)
        return total

    def wait_weights(j):
        pltpu.make_async_copy(wts.at[:, j], wts.at[:, j], wt_sem.at[j]).wait()

    def wait_weights_rem(g):
        pltpu.make_async_copy(wts_rem.at[:, g], wts_rem.at[:, g], wt_sem.at[chans + g]).wait()

    wait_for(st_core.at[1 - core], core_recv.at[0])
    chip_sum = st_core[0] + st_core[1]
    st_own[2] = chip_sum
    st_z[z] = chip_sum

    reach = ((1, nz - 1), (2, nz - 2), tuple(range(3, nz - 2)))
    if nz < 4:
        reach = ((1,), (), ())

    def send_z(step):
        for k in reach[step]:
            send(
                st_own.at[2], st_z.at[z], stat_send.at[3 + k], z_recv.at[k - 1],
                {"strip": to_z(k)},
            )

    def got_z(step):
        for k in reach[step]:
            wait_for(st_z.at[(z + nz - k) % nz], z_recv.at[k - 1])

    prepare_edge(0)
    send_z(0)

    @pl.loop(0, rows)
    def _(q):
        prepare(0, q)

    wait_weights(0)

    for pair in range(pairs):
        add_to(pair, products(pair, (0, 1, 2), (0,), ()), first=True)


    def got(c):
        for d in range(2):
            wait_for(pair_of(1 + d, c), own_recv.at[d, c])

    plan = [
        [(rows + 1 - d, 0, SLAB)]
        + [(2 * i + d, 0, SLAB) for i in range(pairs - 1)]
        + [(rows - 2, d * (SLAB // 2), SLAB // 2), (rows - 1, d * (SLAB // 2), SLAB // 2)]
        for d in range(2)
    ]

    def forward(d, k):
        q, start, number = plan[d][k]
        part = pl.ds(start, number)
        send(
            raw.at[1 + d, q, part], raw.at[3, q, part], fwd_send.at[d, k], fwd_recv.at[d, k],
            {"chan": (right, left)[d]},
        )

    def got_far(k):
        for d in range(2):
            q, start, number = plan[d][k]
            wait_for(raw.at[3, q, pl.ds(start, number)], fwd_recv.at[d, k])

    got(0)
    got(1)
    got(edge)
    for k in range(3):
        for d in range(2):
            forward(d, k)
    got_z(0)
    send_z(1)
    wait_weights(1)
    wait_weights(2)
    wait_weights_rem(0)

    for j in (1, 2):
        prepare_edge(j)
        prepare_pair(j, 0)
        prepare_pair(j, 1)

    def add_sides(pair, *steps):
        add_to(pair, products(pair, steps, (1, 2), (0,)))

    add_sides(0, 0, 1, 2)
    add_sides(1, 0, 1)
    got(2)
    for d in range(2):
        forward(d, 3)

    for j in (1, 2):
        prepare_pair(j, 2)

    add_sides(1, 2)
    add_sides(2, 0, 1)
    got_z(1)
    send_z(2)
    got(3)
    for k in range(4, 6):
        for d in range(2):
            forward(d, k)
    for j in (1, 2):
        prepare_pair(j, 3)

    add_sides(2, 2)
    add_sides(3, 0, 1, 2)

    wait_weights(3)
    wait_weights_rem(1)
    outs = []

    def finish(pair):
        for h in range(2):
            r = 2 * pair + h
            value = raw[0, r].astype(F32) + acc[:, r * width:(r + 1) * width]
            block[r] = jnp.where(r < length, value, 0.0).astype(BF16)

    def put(pair):
        at = pl.ds(2 * pair, 2)
        copy = pltpu.make_async_copy(block.at[at], block_hbm.at[at], out_sem.at[pair])
        copy.start()
        outs.append(copy)

    def both(pair, *steps):
        add_to(pair, products(pair, steps, (3,), (1,)))

    got_far(0)
    prepare_edge(3)
    got_far(1)
    prepare_pair(3, 0)
    both(0, 0, 1)
    got_z(2)
    line_sum = st_z[0]
    for k in range(1, nz):
        line_sum = line_sum + st_z[k]
    st_own[3] = line_sum
    st_y[y] = line_sum

    got_far(2)
    prepare_pair(3, 1)
    for k in range(1, ny):
        send(
            st_own.at[3], st_y.at[y], stat_send.at[2 + nz + k], y_recv.at[k - 1],
            {"strip": to_y(k)},
        )
    both(0, 2)
    finish(0)
    both(1, 0, 1)
    put(0)
    got_far(3)
    prepare_pair(3, 2)
    both(1, 2)
    finish(1)
    both(2, 0, 1)
    put(1)
    got_far(4)
    prepare(3, rows - 2)
    both(2, 2)
    finish(2)
    both(3, 0)
    put(2)
    got_far(5)
    prepare(3, rows - 1)
    both(3, 1, 2)
    finish(3)
    put(3)

    for k in range(1, ny):
        wait_for(st_y.at[(y + ny - k) % ny], y_recv.at[k - 1])
    image_sum = st_y[0]
    for k in range(1, ny):
        image_sum = image_sum + st_y[k]
    moments[...] = image_sum / float(strips * (3 * rows // 4) * width * per_group)
    copy = pltpu.make_async_copy(moments, moments_hbm, small_sem.at[7])
    copy.start()
    outs.append(copy)
    for copy in sends:
        copy.wait_send()
    wait_for(edge_hbm.at[0], edge_send.at[1])

    @pl.when(turns)
    def _():
        wait_for(hop, edge_send.at[2])

    for copy in outs:
        copy.wait()


def spread_kernel(
    rows, width, local, block_hbm, moments_hbm, up_hbm, mean_hbm, square_hbm,
    block, moments, mean_out, square_out, buf, in_sem, out_sem,
):
    takes = []
    for r in range(0, rows, 2):
        at = pl.ds(r, 2)
        copy = pltpu.make_async_copy(block_hbm.at[at], block.at[at], in_sem.at[r // 2])
        copy.start()
        takes.append(copy)
    take = pltpu.make_async_copy(moments_hbm, moments, in_sem.at[rows // 2])
    take.start()
    twice = (
        lax.broadcasted_iota(jnp.int32, (width, 2 * width), 1) // 2
        == lax.broadcasted_iota(jnp.int32, (width, 2 * width), 0)
    ).astype(F32).astype(BF16)
    puts = []
    for r in range(rows):
        if r % 2 == 0:
            takes[r // 2].wait()
        buf[r] = jnp.dot(block[r], twice, preferred_element_type=F32).astype(BF16)
        for a in range(2):
            copy = pltpu.make_async_copy(buf.at[r], up_hbm.at[2 * r + a], out_sem.at[2 * r + a])
            copy.start()
            puts.append(copy)
    groups = mean_out.shape[1]
    take.wait()
    mean_out[...] = moments[0:1, 0:groups]
    square_out[...] = moments[1:2, 0:groups]
    for i, (src, dst) in enumerate(((mean_out, mean_hbm), (square_out, square_hbm))):
        copy = pltpu.make_async_copy(src, dst, out_sem.at[2 * rows + i])
        copy.start()
        puts.append(copy)
    for copy in puts:
        copy.wait()


def per_device(
    activations, weight, gamma, beta, group_map, lengths, stale_edges,
    stale_mean, stale_square, old_mean, old_square,
):
    rows, width, local = activations.shape
    channels = weight.shape[1]
    groups = stale_mean.shape[0]
    strips, chans = lax.axis_size("strip"), lax.axis_size("chan")
    ny, nz = torus(strips)
    pairs = rows // 2

    def turned(v):
        return jnp.swapaxes(v, 1, 2)

    dma = pltpu.SemaphoreType.DMA
    any_space = pl.BlockSpec(memory_space=pl.ANY)
    smem = pl.BlockSpec(memory_space=pltpu.SMEM)
    flops = 2 * rows * width * 9 * channels * local
    block, moments = pl.pallas_call(
        functools.partial(main_kernel, rows, width, strips, chans, channels // groups),
        name="gather_conv",
        out_shape=(
            jax.ShapeDtypeStruct((rows, local, width), BF16),
            jax.ShapeDtypeStruct((8, LANES), F32),
        ),
        in_specs=[any_space] * 6 + [smem] + [any_space] * 4,
        out_specs=(any_space, any_space),
        scratch_shapes=[
            pltpu.VMEM((channels // LANES, LANES), F32),
            pltpu.VMEM((channels // LANES, LANES), F32),
            pltpu.VMEM((channels // LANES, LANES), jnp.int32),
            pltpu.VMEM((1, groups), F32),
            pltpu.VMEM((1, groups), F32),
            pltpu.VMEM((1, groups), F32),
            pltpu.VMEM((1, groups), F32),
            pltpu.VMEM((8, LANES), F32),
            dma((8,)),
            pltpu.VMEM((local, width), BF16),
            pltpu.VMEM((chans, rows + 2, local, width), BF16),
            pltpu.VMEM((chans, 3 * MAIN, (rows + 2) * width), BF16),
            pltpu.VMEM((2, 3 * LANES, (rows + 2) * width), BF16),
            pltpu.VMEM((3, chans, local, 3 * MAIN), BF16),
            pltpu.VMEM((3, 2, local, 3 * LANES), BF16),
            pltpu.VMEM((local, rows * width), F32),
            pltpu.VMEM((rows, local, width), BF16),
            pltpu.VMEM((LANES, LANES), F32),
            pltpu.VMEM((channels, LANES), jnp.int32),
            pltpu.VMEM((2, channels, LANES), F32),
            pltpu.VMEM((4, 8, LANES), F32),
            pltpu.VMEM((chans, 8, LANES), F32),
            pltpu.VMEM((2, 8, LANES), F32),
            pltpu.VMEM((nz, 8, LANES), F32),
            pltpu.VMEM((ny, 8, LANES), F32),
            dma((pairs,)),
            dma((chans + 2,)),
            dma((2, pairs + 1)),
            dma((2, pairs + 1)),
            dma((2, 6)),
            dma((2, 6)),
            dma((3,)),
            dma((3,)),
            dma((3 + nz + ny,)),
            dma((chans - 1,)),
            dma((1,)),
            dma((max(nz - 1, 1),)),
            dma((max(ny - 1, 1),)),
            dma((pairs,)),
        ],
        compiler_params=pltpu.CompilerParams(
            collective_id=0, has_side_effects=True, vmem_limit_bytes=60 * 1024 * 1024
        ),
        cost_estimate=pl.CostEstimate(
            flops=flops, bytes_accessed=weight.size * 2, transcendentals=rows * width * channels
        ),
    )(
        turned(activations), turned(stale_edges), turned(weight),
        gamma.reshape(-1, LANES), beta.reshape(-1, LANES), group_map.reshape(-1, LANES), lengths,
        stale_mean.reshape(1, groups), stale_square.reshape(1, groups), old_mean, old_square,
    )

    upsampled, new_mean, new_square = pl.pallas_call(
        functools.partial(spread_kernel, rows, width, local),
        name="spread",
        out_shape=(
            jax.ShapeDtypeStruct((2 * rows, local, 2 * width), BF16),
            jax.ShapeDtypeStruct((1, groups), F32),
            jax.ShapeDtypeStruct((1, groups), F32),
        ),
        in_specs=[any_space, any_space],
        out_specs=(any_space, any_space, any_space),
        scratch_shapes=[
            pltpu.VMEM((rows, local, width), BF16),
            pltpu.VMEM((8, LANES), F32),
            pltpu.VMEM((1, groups), F32),
            pltpu.VMEM((1, groups), F32),
            pltpu.VMEM((rows, local, 2 * width), BF16),
            dma((pairs + 1,)),
            dma((2 * rows + 2,)),
        ],
        compiler_params=pltpu.CompilerParams(vmem_limit_bytes=60 * 1024 * 1024),
    )(block, moments)
    return turned(upsampled), new_mean.reshape(groups), new_square.reshape(groups)


def solution(mesh):
    in_specs = (
        P("strip", None, "chan"),
        P(None, None, "chan"),
        P(),
        P(),
        P(),
        P("strip"),
        P("strip", None, "chan"),
        P(),
        P(),
        P("strip", None),
        P("strip", None),
    )
    out_specs = (P("strip", None, "chan"), P(), P())
    return jax.shard_map(
        per_device, mesh=mesh, in_specs=in_specs, out_specs=out_specs, check_vma=False
    )
```
